8 devices in a mesh: data: 1 (over z), time: 8 (over y, x, core).
Axes of the slice: x: 2, y: 2, z: 1, core: 2. Of those that a mesh axis runs over, the one named last changes fastest.
Arguments:
- x_init: float32 [32, 16, 256], P('data')
- w_in: bfloat16 [256, 1024], replicated
- w_out: bfloat16 [1024, 256], replicated
- gamma_c: bfloat16 [48, 1024], P('time')
- beta_c: bfloat16 [48, 1024], P('time')
- gamma_u: bfloat16 [48, 1024], P('time')
- beta_u: bfloat16 [48, 1024], P('time')
- step_h: float32 [48], P('time')
- guide_w: float32 [1], replicated
Outputs:
- output: float32 [48, 32, 16, 256], P('time', 'data')
All inputs are finite; a program needn't handle non-finite values.
Results may differ from the reference program's by a relative error of at most 0.00827.
Values are sent between devices in bfloat16 or wider.
A program may use at most 1 GiB of HBM per device.

```python
import jax
import jax.numpy as jnp
from jax import lax

SAMPLES = 32
TOKENS = 16
CHANNELS = 256
HIDDEN = 1024
NUM_STEPS = 48
NUM_SWEEPS = 4


def setup_inputs(seed: int = 0, part: int = 0) -> dict:
    base_key = jax.random.key(seed)
    part_key = jax.random.fold_in(base_key, part)
    sub_keys = jax.random.split(base_key, 8)
    x_init = jax.random.normal(part_key, (SAMPLES, TOKENS, CHANNELS), jnp.float32)
    w_in = (jax.random.normal(sub_keys[0], (CHANNELS, HIDDEN), jnp.float32) * CHANNELS ** -0.5).astype(jnp.bfloat16)
    w_out = (jax.random.normal(sub_keys[1], (HIDDEN, CHANNELS), jnp.float32) * HIDDEN ** -0.5).astype(jnp.bfloat16)
    gamma_c = (0.5 * jax.random.normal(sub_keys[2], (NUM_STEPS, HIDDEN), jnp.float32)).astype(jnp.bfloat16)
    beta_c = (0.5 * jax.random.normal(sub_keys[3], (NUM_STEPS, HIDDEN), jnp.float32)).astype(jnp.bfloat16)
    gamma_u = (0.5 * jax.random.normal(sub_keys[4], (NUM_STEPS, HIDDEN), jnp.float32)).astype(jnp.bfloat16)
    beta_u = (0.5 * jax.random.normal(sub_keys[5], (NUM_STEPS, HIDDEN), jnp.float32)).astype(jnp.bfloat16)
    step_h = jax.random.normal(sub_keys[6], (NUM_STEPS,), jnp.float32) * (0.6 * NUM_STEPS ** -0.5)
    guide_w = jax.random.uniform(sub_keys[7], (1,), jnp.float32, 1.0, 3.0)
    return {"x_init": x_init, "w_in": w_in, "w_out": w_out, "gamma_c": gamma_c, "beta_c": beta_c, "gamma_u": gamma_u, "beta_u": beta_u, "step_h": step_h, "guide_w": guide_w}


def reference(x_init, w_in, w_out, gamma_c, beta_c, gamma_u, beta_u, step_h, guide_w):
    guide = guide_w[0]
    tok_rows = SAMPLES * TOKENS

    def one_step(step_args):
        x_step, cond_gain, cond_shift, unc_gain, unc_shift, h_one = step_args
        pre_act = jnp.dot(x_step.reshape(tok_rows, CHANNELS).astype(jnp.bfloat16), w_in, preferred_element_type=jnp.float32)
        act_c = jax.nn.gelu(pre_act * (1.0 + cond_gain.astype(jnp.float32)) + cond_shift.astype(jnp.float32)).astype(jnp.bfloat16)
        act_u = jax.nn.gelu(pre_act * (1.0 + unc_gain.astype(jnp.float32)) + unc_shift.astype(jnp.float32)).astype(jnp.bfloat16)
        out_c = jnp.dot(act_c, w_out, preferred_element_type=jnp.float32)
        out_u = jnp.dot(act_u, w_out, preferred_element_type=jnp.float32)
        drift = h_one * ((1.0 + guide) * out_c - guide * out_u)
        return drift.reshape(SAMPLES, TOKENS, CHANNELS)

    def sweep(states, unused):
        drifts = lax.map(one_step, (states, gamma_c, beta_c, gamma_u, beta_u, step_h))
        earlier = jnp.cumsum(drifts[:-1], axis=0)
        offsets = jnp.concatenate([jnp.zeros_like(drifts[:1]), earlier], axis=0)
        return x_init[None] + offsets, None

    start = jnp.broadcast_to(x_init[None], (NUM_STEPS, SAMPLES, TOKENS, CHANNELS))
    final, ignored = lax.scan(sweep, start, None, length=NUM_SWEEPS)
    return final
```

```python
import functools
import math

import jax
import jax.numpy as jnp
from jax import lax
from jax.experimental import pallas as pl
from jax.experimental.pallas import tpu as pltpu
from jax.sharding import PartitionSpec as P

NUM_SWEEPS = 4
ROOT = math.sqrt(2.0 / math.pi)
LIN = 2.0 * ROOT
CUB = 8.0 * ROOT * 0.044715
CH = 32
DUO = 2
NCH = 4
NB = NUM_SWEEPS * NCH
OWN = CH * DUO * NCH
STEPS = 6
PAIR = 2 * STEPS
ROWS = PAIR * CH
WIDTH = 256
HIDDEN = 1024
NEED = 3
MESH = pl.DeviceIdType.MESH

dot = functools.partial(jnp.dot, preferred_element_type=jnp.float32)


def half_gelu(pre, gain, shift):
    half = pre * gain + shift
    arg = half * (half * half * CUB + LIN)
    return (half * (1.0 + jnp.tanh(arg))).astype(jnp.bfloat16)


def kernel(x_ref, w_in, w_out, gamma_c, beta_c, gamma_u, beta_u, h_ref, guide_ref, loc_out, base_out, loc, base, par, hvec, sib_par, w1, xb, abuf,
           tbuf, vbuf, rec, sib_send, sib_recv, send_sem, recv_sem, out_send, out_recv):
    time = lax.axis_index("time")
    data = lax.axis_index("data")
    core = lax.rem(time, 2)
    chip = lax.div(time, 2)
    sibling = time + 1 - 2 * core
    row0 = pl.multiple_of(core * OWN, OWN)

    def peer(step):
        return lax.rem(time + 2 * step, 8)

    barrier = pltpu.get_barrier_semaphore()
    for other in (sibling, peer(1), peer(2), peer(3)):
        pl.semaphore_signal(barrier, inc=1, device_id=(data, other), device_id_type=MESH)
    pl.semaphore_wait(barrier, 4)

    def remote(src, dst, send, recv, target):
        return pltpu.make_async_remote_copy(src_ref=src, dst_ref=dst, send_sem=send, recv_sem=recv, device_id=(data, target), device_id_type=MESH)

    own = pl.ds(core * STEPS, STEPS)
    for k in range(STEPS):
        hvec[core * STEPS + k] = jnp.full((8, 128), h_ref[k], jnp.float32)
    raw = [gamma_c, beta_c, gamma_u, beta_u]
    par_copies = [remote(raw[i], sib_par.at[i], sib_send.at[i], sib_recv.at[i], sibling) for i in range(4)]
    par_copies.append(remote(hvec.at[own], hvec.at[own], sib_send.at[4], sib_recv.at[4], sibling))
    for copy in par_copies:
        copy.start()

    def spread(refs, first):
        for i in range(4):
            full = refs[i][...].astype(jnp.float32)
            full = 0.5 * (1.0 + full) if i % 2 == 0 else 0.5 * full
            for k in range(STEPS):
                par[first + k, i] = jnp.broadcast_to(full[k:k + 1], (8, HIDDEN))

    def round_rows(c):
        return pl.ds(pl.multiple_of(row0 + c * (DUO * CH), DUO * CH), DUO * CH)

    spread(raw, core * STEPS)
    for n in range(4):
        w1[n] = w_in[:, 256 * n:256 * n + 256]
    loc[...] = jnp.zeros_like(loc)
    for c in range(NCH):
        base[c] = x_ref[round_rows(c), :].reshape(DUO, CH, WIDTH)
    for copy in par_copies:
        copy.wait()
    spread([sib_par.at[i] for i in range(4)], (1 - core) * STEPS)

    guide = guide_ref[0]

    def stage_x(i, c):
        for t in range(PAIR):
            value = base[c, i] if t == 0 else base[c, i] + loc[t, c, i]
            xb[i, CH * t:CH * t + CH, :] = value.astype(jnp.bfloat16)

    def stage_a(i):
        for n in range(4):
            abuf[i, n] = dot(xb[i], w1[n])

    def gelus(i, n):
        lanes = slice(256 * n, 256 * n + 256)
        cond, free = [], []
        for t in range(PAIR):
            wide = [jnp.concatenate([par[t, p, :, lanes]] * (CH // 8), axis=0) for p in range(4)]
            pre = abuf[i, n, CH * t:CH * t + CH, :]
            cond.append(half_gelu(pre, wide[0], wide[1]))
            free.append(half_gelu(pre, wide[2], wide[3]))
        return jnp.concatenate(cond, axis=0), jnp.concatenate(free, axis=0)

    def stage_f(i, c, event, f_c, f_u):
        total = None
        for t in range(PAIR):
            rows = slice(CH * t, CH * t + CH)
            hk = jnp.concatenate([jnp.concatenate([hvec[t]] * 2, axis=1)] * (CH // 8), axis=0)
            drift = hk * ((1.0 + guide) * f_c[rows] - guide * f_u[rows])
            total = drift if total is None else total + drift
            if t + 1 < PAIR:
                loc[t + 1, c, i] = total
            else:
                tbuf[event, i] = total

    def copy_to(lane, e, src, step):
        return remote(src, rec.at[lane, e], send_sem.at[step - 1, e], recv_sem.at[lane, e], peer(step))

    def send_sum(e):
        @pl.when(chip == 0)
        def _():
            copy_to(0, e, tbuf.at[e], 1).start()

        @pl.when(chip == 2)
        def _():
            copy_to(1, e, tbuf.at[e], 1).start()

    def got(lane, e):
        remote(rec.at[lane, e], rec.at[lane, e], send_sem.at[0, e], recv_sem.at[lane, e], peer(1)).wait_recv()

    def set_base(e, total, last):
        c = lax.rem(e, NCH)
        rows = round_rows(c)
        value = x_ref[rows, :].reshape(DUO, CH, WIDTH)
        if total is not None:
            value = value + total
        if last:
            base_out[rows, :] = value.reshape(DUO * CH, WIDTH)
            remote(base_out.at[rows], base_out.at[rows], out_send.at[1, c], out_recv.at[1, c], sibling).start()
        else:
            base[c] = value

    def take(e, last):
        @pl.when(chip == 1)
        def _():
            got(0, e)
            below = rec[0, e]
            vbuf[e] = below + tbuf[e]
            copy_to(0, e, vbuf.at[e], 1).start()
            copy_to(0, e, vbuf.at[e], 2).start()
            set_base(e, below, last)

        @pl.when(chip == 2)
        def _():
            got(0, e)
            set_base(e, rec[0, e], last)

        @pl.when(chip == 3)
        def _():
            got(0, e)
            got(1, e)
            set_base(e, rec[0, e] + rec[1, e], last)

    def send_local(e):
        c = lax.rem(e, NCH)
        for k in range(STEPS):
            loc_out[k, core * NCH + c] = loc[core * STEPS + k, c]
        local_copy(c).start()

    def local_copy(c):
        return remote(loc.at[pl.ds((1 - core) * STEPS, STEPS), c], loc_out.at[:, core * NCH + c], out_send.at[0, c], out_recv.at[0, c], sibling)

    def one_round(r, carry):
        c = lax.rem(r, NCH)
        c_next = lax.rem(r + 1, NCH)

        @pl.when(r >= 1)
        def _():
            send_sum(r - 1)

        @pl.when((r >= NEED) & (r < NEED + NB - NCH))
        def _():
            take(r - NEED, False)

        @pl.when(r >= NEED + NB - NCH)
        def _():
            take(r - NEED, True)

        @pl.when(r >= NB - NCH + 1)
        def _():
            send_local(r - 1)

        for i in range(DUO):
            follow = (i + 1) % DUO
            stage_x(follow, c if i + 1 < DUO else c_next)
            f_c = f_u = None
            for n in range(4):
                weight = w_out[256 * n:256 * n + 256, :]
                cond, free = gelus(i, n)
                part_c, part_u = dot(cond, weight), dot(free, weight)
                f_c = part_c if n == 0 else f_c + part_c
                f_u = part_u if n == 0 else f_u + part_u
                if n == 1:
                    stage_a(follow)
            stage_f(i, c, r, f_c, f_u)
        return carry

    stage_x(0, 0)
    stage_a(0)
    lax.fori_loop(0, NB, one_round, 0)
    send_sum(NB - 1)
    send_local(NB - 1)

    @pl.when(chip == 0)
    def _():
        for c in range(NCH):
            set_base(c, None, True)

    for e in range(NB - NEED, NB):
        take(e, True)

    def drain(e, carry):
        @pl.when((chip == 0) | (chip == 2))
        def _():
            copy_to(0, e, tbuf.at[e], 1).wait_send()

        @pl.when(chip == 1)
        def _():
            copy_to(0, e, vbuf.at[e], 1).wait_send()
            copy_to(0, e, vbuf.at[e], 2).wait_send()
        return carry

    def finish_out(c, carry):
        rows = round_rows(c)
        local_copy(c).wait()
        remote(base_out.at[rows], base_out.at[rows], out_send.at[1, c], out_recv.at[1, c], sibling).wait()
        return carry

    lax.fori_loop(0, NB, drain, 0)
    lax.fori_loop(0, NCH, finish_out, 0)


def solution(mesh):
    vmem = pl.BlockSpec(memory_space=pltpu.VMEM)
    smem = pl.BlockSpec(memory_space=pltpu.SMEM)
    dma = pltpu.SemaphoreType.DMA

    def local(x_init, w_in, w_out, gamma_c, beta_c, gamma_u, beta_u, step_h, guide_w):
        samples, tokens, width = x_init.shape
        rows = samples * tokens
        loc, base = pl.pallas_call(
            kernel,
            out_shape=(jax.ShapeDtypeStruct((STEPS, 2 * NCH, DUO, CH, width), jnp.float32), jax.ShapeDtypeStruct((rows, width), jnp.float32)),
            in_specs=[vmem] * 7 + [smem] * 2,
            out_specs=(vmem, vmem),
            scratch_shapes=[
                pltpu.VMEM((PAIR, NCH, DUO, CH, WIDTH), jnp.float32),
                pltpu.VMEM((NCH, DUO, CH, WIDTH), jnp.float32),
                pltpu.VMEM((PAIR, 4, 8, HIDDEN), jnp.float32),
                pltpu.VMEM((PAIR, 8, 128), jnp.float32),
                pltpu.VMEM((4, STEPS, HIDDEN), jnp.bfloat16),
                pltpu.VMEM((4, WIDTH, WIDTH), jnp.bfloat16),
                pltpu.VMEM((DUO, ROWS, WIDTH), jnp.bfloat16),
                pltpu.VMEM((DUO, 4, ROWS, WIDTH), jnp.float32),
                pltpu.VMEM((NB, DUO, CH, WIDTH), jnp.float32),
                pltpu.VMEM((NB, DUO, CH, WIDTH), jnp.float32),
                pltpu.VMEM((2, NB, DUO, CH, WIDTH), jnp.float32),
                dma((5,)), dma((5,)), dma((2, NB)), dma((2, NB)), dma((2, NCH)), dma((2, NCH)),
            ],
            compiler_params=pltpu.CompilerParams(collective_id=0, has_side_effects=True, vmem_limit_bytes=48 * 2 ** 20),
            name="picard",
        )(x_init.reshape(rows, width), w_in, w_out, gamma_c, beta_c, gamma_u, beta_u, step_h, guide_w)
        return (base[None] + loc.reshape(STEPS, rows, width)).reshape(STEPS, samples, tokens, width)

    return jax.shard_map(local, mesh=mesh, in_specs=(P("data", None, None), P(None, None), P(None, None), P("time", None), P("time", None), P("time", None), P("time", None), P("time"), P(None)), out_specs=P("time", "data", None, None), check_vma=False)
```

```python
import functools
import math

import jax
import jax.numpy as jnp
from jax import lax
from jax.experimental import pallas as pl
from jax.experimental.pallas import tpu as pltpu
from jax.sharding import PartitionSpec as P

NUM_SWEEPS = 4
ROOT = math.sqrt(2.0 / math.pi)
LIN = 2.0 * ROOT
CUB = 8.0 * ROOT * 0.044715
CH = 32
DUO = 2
NCH = 4
NB = NUM_SWEEPS * NCH
OWN = CH * DUO * NCH
STEPS = 6
PAIR = 2 * STEPS
ROWS = PAIR * CH
WIDTH = 256
HIDDEN = 1024
NEED = 3
PASS = 2
MESH = pl.DeviceIdType.MESH

dot = functools.partial(jnp.dot, preferred_element_type=jnp.float32)


def half_gelu(pre, gain, shift):
    half = pre * gain + shift
    arg = half * (half * half * CUB + LIN)
    return (half * (1.0 + jnp.tanh(arg))).astype(jnp.bfloat16)


def kernel(x_hbm, w_in, w_out_hbm, gamma_c, beta_c, gamma_u, beta_u, h_ref, guide_ref, loc_out, base_out, x_own, w_out, loc, base, par, hvec, own_par,
           sib_par, w1, xb, abuf, tbuf, vbuf, rec, rec_last, in_sem, sib_send, sib_recv, send_sem, recv_sem, out_send, out_recv, last_send, last_recv,
           base_send, base_recv):
    time = lax.axis_index("time")
    data = lax.axis_index("data")
    core = lax.rem(time, 2)
    chip = lax.div(time, 2)
    sibling = time + 1 - 2 * core
    row0 = pl.multiple_of(core * OWN, OWN)

    def peer(step):
        return lax.rem(time + 2 * step, 8)

    raw = [gamma_c, beta_c, gamma_u, beta_u]
    pairs = [(raw[i], own_par.at[i]) for i in range(4)] + [(x_hbm.at[core], x_own)]
    pairs += [(w_in.at[:, pl.ds(256 * n, 256)], w1.at[n]) for n in range(4)] + [(w_out_hbm, w_out)]
    fetches = [pltpu.make_async_copy(src, dst, in_sem.at[i]) for i, (src, dst) in enumerate(pairs)]
    for fetch in fetches:
        fetch.start()

    barrier = pltpu.get_barrier_semaphore()
    for other in (sibling, peer(1), peer(2), peer(3)):
        pl.semaphore_signal(barrier, inc=1, device_id=(data, other), device_id_type=MESH)
    pl.semaphore_wait(barrier, 4)

    def remote(src, dst, send, recv, target):
        return pltpu.make_async_remote_copy(src_ref=src, dst_ref=dst, send_sem=send, recv_sem=recv, device_id=(data, target), device_id_type=MESH)

    own = pl.ds(core * STEPS, STEPS)
    for k in range(STEPS):
        hvec[core * STEPS + k] = jnp.full((8, 128), h_ref[k], jnp.float32)
    for fetch in fetches[:4]:
        fetch.wait()
    par_copies = [remote(own_par.at[i], sib_par.at[i], sib_send.at[i], sib_recv.at[i], sibling) for i in range(4)]
    par_copies.append(remote(hvec.at[own], hvec.at[own], sib_send.at[4], sib_recv.at[4], sibling))
    for copy in par_copies:
        copy.start()

    def spread(refs, first):
        for i in range(4):
            full = refs[i][...].astype(jnp.float32)
            full = 0.5 * (1.0 + full) if i % 2 == 0 else 0.5 * full
            for k in range(STEPS):
                par[first + k, i] = jnp.broadcast_to(full[k:k + 1], (8, HIDDEN))

    def round_rows(c):
        return pl.ds(pl.multiple_of(row0 + c * (DUO * CH), DUO * CH), DUO * CH)

    def stage_x(i, c):
        for t in range(PAIR):
            value = base[c, i] if t == 0 else base[c, i] + loc[t, c, i]
            xb[i, CH * t:CH * t + CH, :] = value.astype(jnp.bfloat16)

    def stage_a(i):
        for n in range(4):
            abuf[i, n] = dot(xb[i], w1[n])

    loc[...] = jnp.zeros_like(loc)
    spread([own_par.at[i] for i in range(4)], core * STEPS)
    for fetch in fetches[4:]:
        fetch.wait()
    base[...] = x_own[...]
    stage_x(0, 0)
    stage_a(0)
    for copy in par_copies:
        copy.wait()
    spread([sib_par.at[i] for i in range(4)], (1 - core) * STEPS)

    guide = guide_ref[0]

    def gelus(i, n):
        lanes = slice(256 * n, 256 * n + 256)
        cond, free = [], []
        for t in range(PAIR):
            wide = [jnp.concatenate([par[t, p, :, lanes]] * (CH // 8), axis=0) for p in range(4)]
            pre = abuf[i, n, CH * t:CH * t + CH, :]
            cond.append(half_gelu(pre, wide[0], wide[1]))
            free.append(half_gelu(pre, wide[2], wide[3]))
        return jnp.concatenate(cond, axis=0), jnp.concatenate(free, axis=0)

    def stage_f(i, c, event, f_c, f_u):
        total = None
        for t in range(PAIR):
            rows = slice(CH * t, CH * t + CH)
            hk = jnp.concatenate([jnp.concatenate([hvec[t]] * 2, axis=1)] * (CH // 8), axis=0)
            drift = hk * ((1.0 + guide) * f_c[rows] - guide * f_u[rows])
            total = drift if total is None else total + drift
            if t + 1 < PAIR:
                loc[t + 1, c, i] = total
            else:
                tbuf[event, i] = total

    def copy_to(lane, e, src, step):
        return remote(src, rec.at[lane, e], send_sem.at[step - 1, e], recv_sem.at[lane, e], peer(step))

    def send_sum(e):
        @pl.when(chip == 0)
        def _():
            copy_to(0, e, tbuf.at[e], 1).start()

        @pl.when(chip == 2)
        def _():
            copy_to(1, e, tbuf.at[e], 1).start()

    def got(lane, e):
        remote(rec.at[lane, e], rec.at[lane, e], send_sem.at[0, e], recv_sem.at[lane, e], peer(1)).wait_recv()

    def set_base(e, total, last):
        c = lax.rem(e, NCH)
        rows = round_rows(c)
        value = x_own[c]
        if total is not None:
            value = value + total
        if last:
            base_out[rows, :] = value.reshape(DUO * CH, WIDTH)
            remote(base_out.at[rows], base_out.at[rows], out_send.at[1, c], out_recv.at[1, c], sibling).start()
        else:
            base[c] = value

    def relay(e, last):
        @pl.when(chip == 1)
        def _():
            got(0, e)
            below = rec[0, e]
            vbuf[e] = below + tbuf[e]
            copy_to(0, e, vbuf.at[e], 1).start()
            copy_to(0, e, vbuf.at[e], 2).start()
            set_base(e, below, last)

    def take(e, last):
        @pl.when(chip == 2)
        def _():
            got(0, e)
            set_base(e, rec[0, e], last)

        @pl.when(chip == 3)
        def _():
            got(0, e)
            got(1, e)
            set_base(e, rec[0, e] + rec[1, e], last)

    def last_copy(source, i, step):
        return remote(tbuf.at[NB - 1, i], rec_last.at[source, i], last_send.at[step - 1, i], last_recv.at[source, i], peer(step))

    def send_last(i):
        for source in range(3):
            @pl.when(chip == source)
            def _():
                for step in range(3 - source, 0, -1):
                    last_copy(source, i, step).start()

    def half_rows(i):
        return pl.ds(pl.multiple_of(row0 + ((NCH - 1) * DUO + i) * CH, CH), CH)

    def base_copy(i):
        return remote(base_out.at[half_rows(i)], base_out.at[half_rows(i)], base_send.at[i], base_recv.at[i], sibling)

    def take_last(i):
        for mine in range(4):
            @pl.when(chip == mine)
            def _():
                value = x_own[NCH - 1, i]
                for source in range(mine):
                    last_copy(source, i, 1).wait_recv()
                    value = value + rec_last[source, i]
                base_out[half_rows(i), :] = value
                base_copy(i).start()

    def send_local(e):
        c = lax.rem(e, NCH)
        for k in range(STEPS):
            loc_out[k, core * NCH + c] = loc[core * STEPS + k, c]
        local_copy(c).start()

    def local_copy(c):
        return remote(loc.at[pl.ds((1 - core) * STEPS, STEPS), c], loc_out.at[:, core * NCH + c], out_send.at[0, c], out_recv.at[0, c], sibling)

    def one_block(i, c, c_after, event):
        follow = (i + 1) % DUO
        stage_x(follow, c_after)
        f_c = f_u = None
        for n in range(4):
            weight = w_out[256 * n:256 * n + 256, :]
            cond, free = gelus(i, n)
            part_c, part_u = dot(cond, weight), dot(free, weight)
            f_c = part_c if n == 0 else f_c + part_c
            f_u = part_u if n == 0 else f_u + part_u
            if n == 1:
                stage_a(follow)
        stage_f(i, c, event, f_c, f_u)

    def one_round(r, carry):
        c = lax.rem(r, NCH)

        @pl.when(r >= 1)
        def _():
            send_sum(r - 1)

        @pl.when((r >= PASS) & (r < PASS + NB - NCH))
        def _():
            relay(r - PASS, False)

        @pl.when(r >= PASS + NB - NCH)
        def _():
            relay(r - PASS, True)

        @pl.when(r >= NEED)
        def _():
            take(r - NEED, False)

        @pl.when(r >= NB - NCH + 1)
        def _():
            send_local(r - 1)

        one_block(0, c, c, r)
        one_block(1, c, lax.rem(r + 1, NCH), r)
        return carry

    lax.fori_loop(0, NB - 1, one_round, 0)
    send_sum(NB - 2)
    relay(NB - 1 - PASS, True)
    take(NB - 1 - NEED, True)
    send_local(NB - 2)

    @pl.when(chip == 0)
    def _():
        for c in range(NCH - 1):
            set_base(c, None, True)

    one_block(0, NCH - 1, NCH - 1, NB - 1)
    send_last(0)
    one_block(1, NCH - 1, 0, NB - 1)
    send_last(1)
    send_local(NB - 1)
    relay(NB - 2, True)
    for e in range(NB - NEED, NB - 1):
        take(e, True)
    take_last(0)
    take_last(1)

    def drain(e, carry):
        @pl.when((chip == 0) | (chip == 2))
        def _():
            copy_to(0, e, tbuf.at[e], 1).wait_send()

        @pl.when(chip == 1)
        def _():
            copy_to(0, e, vbuf.at[e], 1).wait_send()
            copy_to(0, e, vbuf.at[e], 2).wait_send()
        return carry

    def finish_local(c, carry):
        local_copy(c).wait()
        return carry

    def finish_base(c, carry):
        rows = round_rows(c)
        remote(base_out.at[rows], base_out.at[rows], out_send.at[1, c], out_recv.at[1, c], sibling).wait()
        return carry

    lax.fori_loop(0, NB - 1, drain, 0)
    for source in range(3):
        @pl.when(chip == source)
        def _():
            for i in range(DUO):
                for step in range(1, 4 - source):
                    last_copy(source, i, step).wait_send()

    lax.fori_loop(0, NCH, finish_local, 0)
    lax.fori_loop(0, NCH - 1, finish_base, 0)
    base_copy(0).wait()
    base_copy(1).wait()


def solution(mesh):
    vmem = pl.BlockSpec(memory_space=pltpu.VMEM)
    smem = pl.BlockSpec(memory_space=pltpu.SMEM)
    hbm = pl.BlockSpec(memory_space=pltpu.HBM)
    dma = pltpu.SemaphoreType.DMA

    def local(x_init, w_in, w_out, gamma_c, beta_c, gamma_u, beta_u, step_h, guide_w):
        samples, tokens, width = x_init.shape
        rows = samples * tokens
        loc, base = pl.pallas_call(
            kernel,
            out_shape=(jax.ShapeDtypeStruct((STEPS, 2 * NCH, DUO, CH, width), jnp.float32), jax.ShapeDtypeStruct((rows, width), jnp.float32)),
            in_specs=[hbm] * 7 + [smem] * 2,
            out_specs=(vmem, vmem),
            scratch_shapes=[
                pltpu.VMEM((NCH, DUO, CH, WIDTH), jnp.float32),
                pltpu.VMEM((HIDDEN, WIDTH), jnp.bfloat16),
                pltpu.VMEM((PAIR, NCH, DUO, CH, WIDTH), jnp.float32),
                pltpu.VMEM((NCH, DUO, CH, WIDTH), jnp.float32),
                pltpu.VMEM((PAIR, 4, 8, HIDDEN), jnp.float32),
                pltpu.VMEM((PAIR, 8, 128), jnp.float32),
                pltpu.VMEM((4, STEPS, HIDDEN), jnp.bfloat16),
                pltpu.VMEM((4, STEPS, HIDDEN), jnp.bfloat16),
                pltpu.VMEM((4, WIDTH, WIDTH), jnp.bfloat16),
                pltpu.VMEM((DUO, ROWS, WIDTH), jnp.bfloat16),
                pltpu.VMEM((DUO, 4, ROWS, WIDTH), jnp.float32),
                pltpu.VMEM((NB, DUO, CH, WIDTH), jnp.float32),
                pltpu.VMEM((NB, DUO, CH, WIDTH), jnp.float32),
                pltpu.VMEM((2, NB, DUO, CH, WIDTH), jnp.float32),
                pltpu.VMEM((3, DUO, CH, WIDTH), jnp.float32),
                dma((10,)), dma((5,)), dma((5,)), dma((2, NB - 1)), dma((2, NB - 1)), dma((2, NCH)), dma((2, NCH)),
                dma((3, DUO)), dma((3, DUO)), dma((DUO,)), dma((DUO,)),
            ],
            compiler_params=pltpu.CompilerParams(collective_id=0, has_side_effects=True, vmem_limit_bytes=48 * 2 ** 20),
            name="picard",
        )(*(pltpu.with_memory_space_constraint(value, pltpu.HBM) for value in (x_init.reshape(2, NCH, DUO, CH, width), w_in, w_out, gamma_c, beta_c, gamma_u, beta_u)), step_h, guide_w)
        return (base[None] + loc.reshape(STEPS, rows, width)).reshape(STEPS, samples, tokens, width)

    return jax.shard_map(local, mesh=mesh, in_specs=(P("data", None, None), P(None, None), P(None, None), P("time", None), P("time", None), P("time", None), P("time", None), P("time"), P(None)), out_specs=P("time", "data", None, None), check_vma=False)
```

```python
import functools
import math

import jax
import jax.numpy as jnp
from jax import lax
from jax.experimental import pallas as pl
from jax.experimental.pallas import tpu as pltpu
from jax.sharding import PartitionSpec as P

NUM_SWEEPS = 4
ROOT = math.sqrt(2.0 / math.pi)
SCALE = (ROOT * 0.044715) ** (1.0 / 3.0)
LIN = ROOT / SCALE
CH = 32
DUO = 2
NCH = 4
NB = NUM_SWEEPS * NCH
OWN = CH * DUO * NCH
STEPS = 6
PAIR = 2 * STEPS
ROWS = PAIR * CH
WIDTH = 256
HIDDEN = 1024
NEED = 3
PASS = 2
AHEAD = ({0: (0,), 1: (1,), 2: (2,), 3: (3,)}, {0: (0,), 1: (1,), 2: (2,), 3: (3,)})
MESH = pl.DeviceIdType.MESH

dot = functools.partial(jnp.dot, preferred_element_type=jnp.float32)


def scaled_gelu(pre, gain, shift):
    y = pre * gain + shift
    return (y * (1.0 + jnp.tanh(y * (y * y + LIN)))).astype(jnp.bfloat16)


def kernel(x_hbm, w_in, w_out_hbm, gamma_c, beta_c, gamma_u, beta_u, h_hbm, guide_ref, loc_out, base_out, h_ref, x_own, w_out, loc, base, par, hvec, own_par,
           sib_par, w1, xb, abuf, tbuf, vbuf, rec, rec_last, in_sem, sib_send, sib_recv, send_sem, recv_sem, out_send, out_recv, last_send, last_recv,
           base_send, base_recv):
    time = lax.axis_index("time")
    data = lax.axis_index("data")
    core = lax.rem(time, 2)
    chip = lax.div(time, 2)
    sibling = time + 1 - 2 * core
    row0 = pl.multiple_of(core * OWN, OWN)

    def peer(step):
        return lax.rem(time + 2 * step, 8)

    raw = [gamma_c, beta_c, gamma_u, beta_u]
    pairs = [(raw[i], own_par.at[i]) for i in range(4)] + [(h_hbm, h_ref), (x_hbm.at[core], x_own)]
    pairs += [(w_in.at[:, pl.ds(256 * n, 256)], w1.at[n]) for n in range(4)] + [(w_out_hbm, w_out)]
    fetches = [pltpu.make_async_copy(src, dst, in_sem.at[i]) for i, (src, dst) in enumerate(pairs)]
    for fetch in fetches:
        fetch.start()

    barrier = pltpu.get_barrier_semaphore()
    for other in (sibling, peer(1), peer(2), peer(3)):
        pl.semaphore_signal(barrier, inc=1, device_id=(data, other), device_id_type=MESH)
    pl.semaphore_wait(barrier, 4)

    def remote(src, dst, send, recv, target):
        return pltpu.make_async_remote_copy(src_ref=src, dst_ref=dst, send_sem=send, recv_sem=recv, device_id=(data, target), device_id_type=MESH)

    own = pl.ds(core * STEPS, STEPS)
    for fetch in fetches[:5]:
        fetch.wait()
    for k in range(STEPS):
        hvec[core * STEPS + k] = jnp.full((8, 128), h_ref[k] * (0.5 / SCALE), jnp.float32)
    par_copies = [remote(own_par.at[i], sib_par.at[i], sib_send.at[i], sib_recv.at[i], sibling) for i in range(4)]
    par_copies.append(remote(hvec.at[own], hvec.at[own], sib_send.at[4], sib_recv.at[4], sibling))
    for copy in par_copies:
        copy.start()

    def spread(refs, first):
        for i in range(4):
            full = refs[i][...].astype(jnp.float32)
            full = SCALE * (1.0 + full) if i % 2 == 0 else SCALE * full
            for k in range(STEPS):
                par[first + k, i] = jnp.broadcast_to(full[k:k + 1], (8, HIDDEN))

    def round_rows(c):
        return pl.ds(pl.multiple_of(row0 + c * (DUO * CH), DUO * CH), DUO * CH)

    def stage_x(i, c):
        for t in range(PAIR):
            value = base[c, i] if t == 0 else base[c, i] + loc[t, c, i]
            xb[i, CH * t:CH * t + CH, :] = value.astype(jnp.bfloat16)

    def stage_a(i, tiles=range(4)):
        for n in tiles:
            abuf[i, n] = dot(xb[i], w1[n])

    loc[...] = jnp.zeros_like(loc)
    spread([own_par.at[i] for i in range(4)], core * STEPS)
    for fetch in fetches[5:]:
        fetch.wait()
    base[...] = x_own[...]
    stage_x(0, 0)
    stage_a(0)
    for copy in par_copies:
        copy.wait()
    spread([sib_par.at[i] for i in range(4)], (1 - core) * STEPS)

    guide = guide_ref[0]

    def gelus(i, n):
        lanes = slice(256 * n, 256 * n + 256)
        cond, free = [], []
        for t in range(PAIR):
            wide = [jnp.concatenate([par[t, p, :, lanes]] * (CH // 8), axis=0) for p in range(4)]
            pre = abuf[i, n, CH * t:CH * t + CH, :]
            cond.append(scaled_gelu(pre, wide[0], wide[1]))
            free.append(scaled_gelu(pre, wide[2], wide[3]))
        return jnp.concatenate(cond, axis=0), jnp.concatenate(free, axis=0)

    def stage_f(i, c, event, f_c, f_u):
        total = None
        for t in range(PAIR):
            rows = slice(CH * t, CH * t + CH)
            hk = jnp.concatenate([jnp.concatenate([hvec[t]] * 2, axis=1)] * (CH // 8), axis=0)
            drift = hk * ((1.0 + guide) * f_c[rows] - guide * f_u[rows])
            total = drift if total is None else total + drift
            if t + 1 < PAIR:
                loc[t + 1, c, i] = total
            else:
                tbuf[event, i] = total

    def copy_to(lane, e, src, step):
        return remote(src, rec.at[lane, e], send_sem.at[step - 1, e], recv_sem.at[lane, e], peer(step))

    def send_sum(e):
        @pl.when(chip == 0)
        def _():
            copy_to(0, e, tbuf.at[e], 1).start()

        @pl.when(chip == 2)
        def _():
            copy_to(1, e, tbuf.at[e], 1).start()

    def got(lane, e):
        remote(rec.at[lane, e], rec.at[lane, e], send_sem.at[0, e], recv_sem.at[lane, e], peer(1)).wait_recv()

    def set_base(e, total, last):
        c = lax.rem(e, NCH)
        rows = round_rows(c)
        value = x_own[c]
        if total is not None:
            value = value + total
        if last:
            base_out[rows, :] = value.reshape(DUO * CH, WIDTH)
            remote(base_out.at[rows], base_out.at[rows], out_send.at[1, c], out_recv.at[1, c], sibling).start()
        else:
            base[c] = value

    def relay(e, last):
        @pl.when(chip == 1)
        def _():
            got(0, e)
            below = rec[0, e]
            vbuf[e] = below + tbuf[e]
            copy_to(0, e, vbuf.at[e], 1).start()
            copy_to(0, e, vbuf.at[e], 2).start()
            set_base(e, below, last)

    def take(e, last):
        @pl.when(chip == 2)
        def _():
            got(0, e)
            set_base(e, rec[0, e], last)

        @pl.when(chip == 3)
        def _():
            got(0, e)
            got(1, e)
            set_base(e, rec[0, e] + rec[1, e], last)

    def last_copy(source, i, step):
        return remote(tbuf.at[NB - 1, i], rec_last.at[source, i], last_send.at[step - 1, i], last_recv.at[source, i], peer(step))

    def send_last(i):
        for source in range(3):
            @pl.when(chip == source)
            def _():
                for step in range(3 - source, 0, -1):
                    last_copy(source, i, step).start()

    def half_rows(i):
        return pl.ds(pl.multiple_of(row0 + ((NCH - 1) * DUO + i) * CH, CH), CH)

    def base_copy(i):
        return remote(base_out.at[half_rows(i)], base_out.at[half_rows(i)], base_send.at[i], base_recv.at[i], sibling)

    def take_last(i):
        for mine in range(4):
            @pl.when(chip == mine)
            def _():
                value = x_own[NCH - 1, i]
                for source in range(mine):
                    last_copy(source, i, 1).wait_recv()
                    value = value + rec_last[source, i]
                base_out[half_rows(i), :] = value
                base_copy(i).start()

    def send_local(e):
        c = lax.rem(e, NCH)
        for k in range(STEPS):
            loc_out[k, core * NCH + c] = loc[core * STEPS + k, c]
        local_copy(c).start()

    def local_copy(c):
        return remote(loc.at[pl.ds((1 - core) * STEPS, STEPS), c], loc_out.at[:, core * NCH + c], out_send.at[0, c], out_recv.at[0, c], sibling)

    def one_block(i, c, c_after, event):
        follow = (i + 1) % DUO
        stage_x(follow, c_after)
        f_c = f_u = None
        for n in range(4):
            weight = w_out[256 * n:256 * n + 256, :]
            cond, free = gelus(i, n)
            part_c, part_u = dot(cond, weight), dot(free, weight)
            f_c = part_c if n == 0 else f_c + part_c
            f_u = part_u if n == 0 else f_u + part_u
            if n in AHEAD[i]:
                stage_a(follow, AHEAD[i][n])
        stage_f(i, c, event, f_c, f_u)

    def one_round(r, carry):
        c = lax.rem(r, NCH)

        @pl.when(r >= 1)
        def _():
            send_sum(r - 1)

        @pl.when((r >= PASS) & (r < PASS + NB - NCH))
        def _():
            relay(r - PASS, False)

        @pl.when(r >= PASS + NB - NCH)
        def _():
            relay(r - PASS, True)

        @pl.when(r >= NEED)
        def _():
            take(r - NEED, False)

        @pl.when(r >= NB - NCH + 1)
        def _():
            send_local(r - 1)

        one_block(0, c, c, r)
        one_block(1, c, lax.rem(r + 1, NCH), r)
        return carry

    lax.fori_loop(0, NB - 1, one_round, 0)
    send_sum(NB - 2)
    relay(NB - 1 - PASS, True)
    take(NB - 1 - NEED, True)
    send_local(NB - 2)

    @pl.when(chip == 0)
    def _():
        for c in range(NCH - 1):
            set_base(c, None, True)

    one_block(0, NCH - 1, NCH - 1, NB - 1)
    send_last(0)
    one_block(1, NCH - 1, 0, NB - 1)
    send_last(1)
    send_local(NB - 1)
    relay(NB - 2, True)
    for e in range(NB - NEED, NB - 1):
        take(e, True)
    take_last(0)
    take_last(1)

    def drain(e, carry):
        @pl.when((chip == 0) | (chip == 2))
        def _():
            copy_to(0, e, tbuf.at[e], 1).wait_send()

        @pl.when(chip == 1)
        def _():
            copy_to(0, e, vbuf.at[e], 1).wait_send()
            copy_to(0, e, vbuf.at[e], 2).wait_send()
        return carry

    def finish_local(c, carry):
        local_copy(c).wait()
        return carry

    def finish_base(c, carry):
        rows = round_rows(c)
        remote(base_out.at[rows], base_out.at[rows], out_send.at[1, c], out_recv.at[1, c], sibling).wait()
        return carry

    lax.fori_loop(0, NB - 1, drain, 0)
    for source in range(3):
        @pl.when(chip == source)
        def _():
            for i in range(DUO):
                for step in range(1, 4 - source):
                    last_copy(source, i, step).wait_send()

    lax.fori_loop(0, NCH, finish_local, 0)
    lax.fori_loop(0, NCH - 1, finish_base, 0)
    base_copy(0).wait()
    base_copy(1).wait()


def solution(mesh):
    vmem = pl.BlockSpec(memory_space=pltpu.VMEM)
    smem = pl.BlockSpec(memory_space=pltpu.SMEM)
    hbm = pl.BlockSpec(memory_space=pltpu.HBM)
    dma = pltpu.SemaphoreType.DMA

    def local(x_init, w_in, w_out, gamma_c, beta_c, gamma_u, beta_u, step_h, guide_w):
        samples, tokens, width = x_init.shape
        rows = samples * tokens
        loc, base = pl.pallas_call(
            kernel,
            out_shape=(jax.ShapeDtypeStruct((STEPS, 2 * NCH, DUO, CH, width), jnp.float32), jax.ShapeDtypeStruct((rows, width), jnp.float32)),
            in_specs=[hbm] * 8 + [smem],
            out_specs=(vmem, vmem),
            scratch_shapes=[
                pltpu.SMEM((STEPS,), jnp.float32),
                pltpu.VMEM((NCH, DUO, CH, WIDTH), jnp.float32),
                pltpu.VMEM((HIDDEN, WIDTH), jnp.bfloat16),
                pltpu.VMEM((PAIR, NCH, DUO, CH, WIDTH), jnp.float32),
                pltpu.VMEM((NCH, DUO, CH, WIDTH), jnp.float32),
                pltpu.VMEM((PAIR, 4, 8, HIDDEN), jnp.float32),
                pltpu.VMEM((PAIR, 8, 128), jnp.float32),
                pltpu.VMEM((4, STEPS, HIDDEN), jnp.bfloat16),
                pltpu.VMEM((4, STEPS, HIDDEN), jnp.bfloat16),
                pltpu.VMEM((4, WIDTH, WIDTH), jnp.bfloat16),
                pltpu.VMEM((DUO, ROWS, WIDTH), jnp.bfloat16),
                pltpu.VMEM((DUO, 4, ROWS, WIDTH), jnp.float32),
                pltpu.VMEM((NB, DUO, CH, WIDTH), jnp.float32),
                pltpu.VMEM((NB, DUO, CH, WIDTH), jnp.float32),
                pltpu.VMEM((2, NB, DUO, CH, WIDTH), jnp.float32),
                pltpu.VMEM((3, DUO, CH, WIDTH), jnp.float32),
                dma((11,)), dma((5,)), dma((5,)), dma((2, NB - 1)), dma((2, NB - 1)), dma((2, NCH)), dma((2, NCH)),
                dma((3, DUO)), dma((3, DUO)), dma((DUO,)), dma((DUO,)),
            ],
            compiler_params=pltpu.CompilerParams(collective_id=0, has_side_effects=True, vmem_limit_bytes=48 * 2 ** 20),
            name="picard",
        )(*(pltpu.with_memory_space_constraint(value, pltpu.HBM) for value in (x_init.reshape(2, NCH, DUO, CH, width), w_in, w_out, gamma_c, beta_c, gamma_u, beta_u, step_h)), guide_w)
        return (base[None] + loc.reshape(STEPS, rows, width)).reshape(STEPS, samples, tokens, width)

    return jax.shard_map(local, mesh=mesh, in_specs=(P("data", None, None), P(None, None), P(None, None), P("time", None), P("time", None), P("time", None), P("time", None), P("time"), P(None)), out_specs=P("time", "data", None, None), check_vma=False)
```

```python
import functools
import math

import jax
import jax.numpy as jnp
from jax import lax
from jax.experimental import pallas as pl
from jax.experimental.pallas import tpu as pltpu
from jax.sharding import PartitionSpec as P

NUM_SWEEPS = 4
ROOT = math.sqrt(2.0 / math.pi)
SCALE = (ROOT * 0.044715) ** (1.0 / 3.0)
LIN = ROOT / SCALE
CH = 32
DUO = 2
NCH = 4
NB = NUM_SWEEPS * NCH
OWN = CH * DUO * NCH
STEPS = 6
PAIR = 2 * STEPS
ROWS = PAIR * CH
WIDTH = 256
PIECES = 8
HIDDEN = 1024
NEED = 3
PASS = 2
AHEAD = ({1: (0,), 2: (1, 2), 3: (3,)}, {1: (0,), 2: (1, 2), 3: (3,)})
MESH = pl.DeviceIdType.MESH

dot = functools.partial(jnp.dot, preferred_element_type=jnp.float32)


def scaled_gelu(pre, gain, shift):
    y = pre * gain + shift
    return (y * (1.0 + jnp.tanh(y * (y * y + LIN)))).astype(jnp.bfloat16)


def kernel(x_hbm, w_in, w_out_hbm, gamma_c, beta_c, gamma_u, beta_u, h_hbm, guide_ref, loc_out, base_out, h_ref, x_own, w_out, loc, base, par, hvec, own_par,
           sib_par, w1, xb, abuf, tbuf, vbuf, rec, rec_last, in_sem, sib_send, sib_recv, send_sem, recv_sem, out_send, out_recv, last_send, last_recv,
           base_send, base_recv):
    time = lax.axis_index("time")
    data = lax.axis_index("data")
    core = lax.rem(time, 2)
    chip = lax.div(time, 2)
    sibling = time + 1 - 2 * core
    row0 = pl.multiple_of(core * OWN, OWN)

    def peer(step):
        return lax.rem(time + 2 * step, 8)

    raw = [gamma_c, beta_c, gamma_u, beta_u]
    pairs = [(raw[i], own_par.at[i]) for i in range(4)] + [(h_hbm, h_ref), (x_hbm.at[core], x_own)]
    pairs += [(w_in.at[:, pl.ds(256 * n, 256)], w1.at[n]) for n in range(4)] + [(w_out_hbm, w_out)]
    fetches = [pltpu.make_async_copy(src, dst, in_sem.at[i]) for i, (src, dst) in enumerate(pairs)]
    for fetch in fetches:
        fetch.start()

    barrier = pltpu.get_barrier_semaphore()
    for other in (sibling, peer(1), peer(2), peer(3)):
        pl.semaphore_signal(barrier, inc=1, device_id=(data, other), device_id_type=MESH)
    pl.semaphore_wait(barrier, 4)

    def remote(src, dst, send, recv, target):
        return pltpu.make_async_remote_copy(src_ref=src, dst_ref=dst, send_sem=send, recv_sem=recv, device_id=(data, target), device_id_type=MESH)

    own = pl.ds(core * STEPS, STEPS)
    for fetch in fetches[:5]:
        fetch.wait()
    for k in range(STEPS):
        hvec[core * STEPS + k] = jnp.full((8, 128), h_ref[k] * (0.5 / SCALE), jnp.float32)
    par_copies = [remote(own_par.at[i], sib_par.at[i], sib_send.at[i], sib_recv.at[i], sibling) for i in range(4)]
    par_copies.append(remote(hvec.at[own], hvec.at[own], sib_send.at[4], sib_recv.at[4], sibling))
    for copy in par_copies:
        copy.start()

    def spread(refs, first):
        for i in range(4):
            full = refs[i][...].astype(jnp.float32)
            full = SCALE * (1.0 + full) if i % 2 == 0 else SCALE * full
            for k in range(STEPS):
                par[first + k, i] = jnp.broadcast_to(full[k:k + 1], (8, HIDDEN))

    def round_rows(c):
        return pl.ds(pl.multiple_of(row0 + c * (DUO * CH), DUO * CH), DUO * CH)

    def stage_x(i, c):
        for t in range(PAIR):
            value = base[c, i] if t == 0 else base[c, i] + loc[t, c, i]
            xb[i, CH * t:CH * t + CH, :] = value.astype(jnp.bfloat16)

    def stage_a(i, tiles=range(4)):
        for n in tiles:
            abuf[i, n] = dot(xb[i], w1[n])

    loc[...] = jnp.zeros_like(loc)
    spread([own_par.at[i] for i in range(4)], core * STEPS)
    for fetch in fetches[5:]:
        fetch.wait()
    base[...] = x_own[...]
    stage_x(0, 0)
    stage_a(0)
    for copy in par_copies:
        copy.wait()
    spread([sib_par.at[i] for i in range(4)], (1 - core) * STEPS)

    guide = guide_ref[0]

    def gelus(i, n):
        lanes = slice(256 * n, 256 * n + 256)
        cond, free = [], []
        for t in range(PAIR):
            wide = [jnp.concatenate([par[t, p, :, lanes]] * (CH // 8), axis=0) for p in range(4)]
            pre = abuf[i, n, CH * t:CH * t + CH, :]
            cond.append(scaled_gelu(pre, wide[0], wide[1]))
            free.append(scaled_gelu(pre, wide[2], wide[3]))
        return jnp.concatenate(cond, axis=0), jnp.concatenate(free, axis=0)

    def stage_f(i, c, event, f_c, f_u):
        total = None
        for t in range(PAIR):
            rows = slice(CH * t, CH * t + CH)
            hk = jnp.concatenate([jnp.concatenate([hvec[t]] * 2, axis=1)] * (CH // 8), axis=0)
            drift = hk * ((1.0 + guide) * f_c[rows] - guide * f_u[rows])
            total = drift if total is None else total + drift
            if t + 1 < PAIR:
                loc[t + 1, c, i] = total
            else:
                tbuf[event, i] = total

    def copy_to(lane, e, src, step):
        return remote(src, rec.at[lane, e], send_sem.at[step - 1, e], recv_sem.at[lane, e], peer(step))

    def send_sum(e):
        @pl.when(chip == 0)
        def _():
            copy_to(0, e, tbuf.at[e], 1).start()

        @pl.when(chip == 2)
        def _():
            copy_to(1, e, tbuf.at[e], 1).start()

    def got(lane, e):
        remote(rec.at[lane, e], rec.at[lane, e], send_sem.at[0, e], recv_sem.at[lane, e], peer(1)).wait_recv()

    def set_base(e, total, last):
        c = lax.rem(e, NCH)
        rows = round_rows(c)
        value = x_own[c]
        if total is not None:
            value = value + total
        if last:
            base_out[rows, :] = value.reshape(DUO * CH, WIDTH)
            remote(base_out.at[rows], base_out.at[rows], out_send.at[1, c], out_recv.at[1, c], sibling).start()
        else:
            base[c] = value

    def relay(e, last):
        @pl.when(chip == 1)
        def _():
            got(0, e)
            below = rec[0, e]
            vbuf[e] = below + tbuf[e]
            copy_to(0, e, vbuf.at[e], 1).start()
            copy_to(0, e, vbuf.at[e], 2).start()
            set_base(e, below, last)

    def take(e, last):
        @pl.when(chip == 2)
        def _():
            got(0, e)
            set_base(e, rec[0, e], last)

        @pl.when(chip == 3)
        def _():
            got(0, e)
            got(1, e)
            set_base(e, rec[0, e] + rec[1, e], last)

    def last_copy(source, i, step):
        return remote(tbuf.at[NB - 1, i], rec_last.at[source, i], last_send.at[step - 1, i], last_recv.at[source, i], peer(step))

    def send_last(i):
        for source in range(3):
            @pl.when(chip == source)
            def _():
                for step in range(3 - source, 0, -1):
                    last_copy(source, i, step).start()

    def half_rows(i):
        return pl.ds(pl.multiple_of(row0 + ((NCH - 1) * DUO + i) * CH, CH), CH)

    def base_copy(i):
        return remote(base_out.at[half_rows(i)], base_out.at[half_rows(i)], base_send.at[i], base_recv.at[i], sibling)

    def take_last(i):
        for mine in range(4):
            @pl.when(chip == mine)
            def _():
                value = x_own[NCH - 1, i]
                for source in range(mine):
                    last_copy(source, i, 1).wait_recv()
                    value = value + rec_last[source, i]
                base_out[half_rows(i), :] = value
                base_copy(i).start()

    def send_local(e):
        c = lax.rem(e, NCH)
        for k in range(STEPS):
            loc_out[k, core * NCH + c] = loc[core * STEPS + k, c]
        local_copy(c).start()

    def local_copy(c):
        return remote(loc.at[pl.ds((1 - core) * STEPS, STEPS), c], loc_out.at[:, core * NCH + c], out_send.at[0, c], out_recv.at[0, c], sibling)

    def one_block(i, c, c_after, event):
        follow = (i + 1) % DUO
        stage_x(follow, c_after)
        f_c = f_u = None
        for n in range(4):
            weight = w_out[256 * n:256 * n + 256, :]
            cond, free = gelus(i, n)
            part_c, part_u = dot(cond, weight), dot(free, weight)
            f_c = part_c if n == 0 else f_c + part_c
            f_u = part_u if n == 0 else f_u + part_u
            if n in AHEAD[i]:
                stage_a(follow, AHEAD[i][n])
        stage_f(i, c, event, f_c, f_u)

    def one_round(r, carry):
        c = lax.rem(r, NCH)

        @pl.when(r >= 1)
        def _():
            send_sum(r - 1)

        @pl.when((r >= PASS) & (r < PASS + NB - NCH))
        def _():
            relay(r - PASS, False)

        @pl.when(r >= PASS + NB - NCH)
        def _():
            relay(r - PASS, True)

        @pl.when(r >= NEED)
        def _():
            take(r - NEED, False)

        @pl.when(r >= NB - NCH + 1)
        def _():
            send_local(r - 1)

        one_block(0, c, c, r)
        one_block(1, c, lax.rem(r + 1, NCH), r)
        return carry

    lax.fori_loop(0, NB - 1, one_round, 0)
    send_sum(NB - 2)
    relay(NB - 1 - PASS, True)
    take(NB - 1 - NEED, True)
    send_local(NB - 2)

    @pl.when(chip == 0)
    def _():
        for c in range(NCH - 1):
            set_base(c, None, True)

    one_block(0, NCH - 1, NCH - 1, NB - 1)
    send_last(0)
    one_block(1, NCH - 1, 0, NB - 1)
    send_last(1)
    send_local(NB - 1)
    relay(NB - 2, True)
    for e in range(NB - NEED, NB - 1):
        take(e, True)
    take_last(0)
    take_last(1)

    def drain(e, carry):
        @pl.when((chip == 0) | (chip == 2))
        def _():
            copy_to(0, e, tbuf.at[e], 1).wait_send()

        @pl.when(chip == 1)
        def _():
            copy_to(0, e, vbuf.at[e], 1).wait_send()
            copy_to(0, e, vbuf.at[e], 2).wait_send()
        return carry

    def finish_local(c, carry):
        local_copy(c).wait()
        return carry

    def finish_base(c, carry):
        rows = round_rows(c)
        remote(base_out.at[rows], base_out.at[rows], out_send.at[1, c], out_recv.at[1, c], sibling).wait()
        return carry

    lax.fori_loop(0, NB - 1, drain, 0)
    for source in range(3):
        @pl.when(chip == source)
        def _():
            for i in range(DUO):
                for step in range(1, 4 - source):
                    last_copy(source, i, step).wait_send()

    lax.fori_loop(0, NCH, finish_local, 0)
    lax.fori_loop(0, NCH - 1, finish_base, 0)
    base_copy(0).wait()
    base_copy(1).wait()


def finish(loc_ref, base_ref, out_hbm, stage, sem):
    pieces = []
    for piece in range(PIECES):
        rows = pl.ds(piece * (2 * OWN // PIECES), 2 * OWN // PIECES)
        for k in range(STEPS):
            stage[k, rows, :] = base_ref[rows, :] + loc_ref[k, rows, :]
        pieces.append(pltpu.make_async_copy(stage.at[:, rows], out_hbm.at[:, rows], sem.at[piece]))
        pieces[-1].start()
    for copy in pieces:
        copy.wait()


def solution(mesh):
    vmem = pl.BlockSpec(memory_space=pltpu.VMEM)
    smem = pl.BlockSpec(memory_space=pltpu.SMEM)
    hbm = pl.BlockSpec(memory_space=pltpu.HBM)
    dma = pltpu.SemaphoreType.DMA

    def local(x_init, w_in, w_out, gamma_c, beta_c, gamma_u, beta_u, step_h, guide_w):
        samples, tokens, width = x_init.shape
        rows = samples * tokens
        loc, base = pl.pallas_call(
            kernel,
            out_shape=(jax.ShapeDtypeStruct((STEPS, 2 * NCH, DUO, CH, width), jnp.float32), jax.ShapeDtypeStruct((rows, width), jnp.float32)),
            in_specs=[hbm] * 8 + [smem],
            out_specs=(vmem, vmem),
            scratch_shapes=[
                pltpu.SMEM((STEPS,), jnp.float32),
                pltpu.VMEM((NCH, DUO, CH, WIDTH), jnp.float32),
                pltpu.VMEM((HIDDEN, WIDTH), jnp.bfloat16),
                pltpu.VMEM((PAIR, NCH, DUO, CH, WIDTH), jnp.float32),
                pltpu.VMEM((NCH, DUO, CH, WIDTH), jnp.float32),
                pltpu.VMEM((PAIR, 4, 8, HIDDEN), jnp.float32),
                pltpu.VMEM((PAIR, 8, 128), jnp.float32),
                pltpu.VMEM((4, STEPS, HIDDEN), jnp.bfloat16),
                pltpu.VMEM((4, STEPS, HIDDEN), jnp.bfloat16),
                pltpu.VMEM((4, WIDTH, WIDTH), jnp.bfloat16),
                pltpu.VMEM((DUO, ROWS, WIDTH), jnp.bfloat16),
                pltpu.VMEM((DUO, 4, ROWS, WIDTH), jnp.float32),
                pltpu.VMEM((NB, DUO, CH, WIDTH), jnp.float32),
                pltpu.VMEM((NB, DUO, CH, WIDTH), jnp.float32),
                pltpu.VMEM((2, NB, DUO, CH, WIDTH), jnp.float32),
                pltpu.VMEM((3, DUO, CH, WIDTH), jnp.float32),
                dma((11,)), dma((5,)), dma((5,)), dma((2, NB - 1)), dma((2, NB - 1)), dma((2, NCH)), dma((2, NCH)),
                dma((3, DUO)), dma((3, DUO)), dma((DUO,)), dma((DUO,)),
            ],
            compiler_params=pltpu.CompilerParams(collective_id=0, has_side_effects=True, vmem_limit_bytes=48 * 2 ** 20),
            name="picard",
        )(*(pltpu.with_memory_space_constraint(value, pltpu.HBM) for value in (x_init.reshape(2, NCH, DUO, CH, width), w_in, w_out, gamma_c, beta_c, gamma_u, beta_u, step_h)), guide_w)
        out = pl.pallas_call(
            finish,
            out_shape=jax.ShapeDtypeStruct((STEPS, rows, width), jnp.float32),
            in_specs=[vmem] * 2,
            out_specs=hbm,
            scratch_shapes=[pltpu.VMEM((STEPS, rows, width), jnp.float32), dma((PIECES,))],
            compiler_params=pltpu.CompilerParams(vmem_limit_bytes=8 * 2 ** 20),
            name="finish",
        )(loc.reshape(STEPS, rows, width), base)
        return out.reshape(STEPS, samples, tokens, width)

    return jax.shard_map(local, mesh=mesh, in_specs=(P("data", None, None), P(None, None), P(None, None), P("time", None), P("time", None), P("time", None), P("time", None), P("time"), P(None)), out_specs=P("time", "data", None, None), check_vma=False)
```

```python
import functools
import math

import jax
import jax.numpy as jnp
from jax import lax
from jax.experimental import pallas as pl
from jax.experimental.pallas import tpu as pltpu
from jax.sharding import PartitionSpec as P

NUM_SWEEPS = 4
ROOT = math.sqrt(2.0 / math.pi)
SCALE = (ROOT * 0.044715) ** (1.0 / 3.0)
LIN = ROOT / SCALE
CH = 32
DUO = 2
NCH = 4
NB = NUM_SWEEPS * NCH
OWN = CH * DUO * NCH
STEPS = 6
PAIR = 2 * STEPS
ROWS = PAIR * CH
WIDTH = 256
PIECES = 8
HIDDEN = 1024
NEED = 3
PASS = 2
AHEAD = ({1: (0,), 2: (1, 2), 3: (3,)}, {1: (0,), 2: (1, 2), 3: (3,)})
MESH = pl.DeviceIdType.MESH

dot = functools.partial(jnp.dot, preferred_element_type=jnp.float32)


def scaled_gelu(pre, gain, shift):
    y = pre * gain + shift
    return (y * (1.0 + jnp.tanh(y * (y * y + LIN)))).astype(jnp.bfloat16)


def kernel(x_hbm, w_in, w_out_hbm, gamma_c, beta_c, gamma_u, beta_u, h_hbm, guide_ref, loc_out, base_out, h_ref, x_own, w_out, loc, base, par, hvec, own_par,
           sib_par, w1, xb, abuf, tbuf, vbuf, rec, rec_early, rec_last, in_sem, sib_send, sib_recv, send_sem, recv_sem, out_send, out_recv, last_send, last_recv,
           base_send, base_recv, early_send, early_recv):
    time = lax.axis_index("time")
    data = lax.axis_index("data")
    core = lax.rem(time, 2)
    chip = lax.div(time, 2)
    sibling = time + 1 - 2 * core
    row0 = pl.multiple_of(core * OWN, OWN)

    def peer(step):
        return lax.rem(time + 2 * step, 8)

    raw = [gamma_c, beta_c, gamma_u, beta_u]
    pairs = [(raw[i], own_par.at[i]) for i in range(4)] + [(h_hbm, h_ref), (x_hbm.at[core], x_own)]
    pairs += [(w_in.at[:, pl.ds(256 * n, 256)], w1.at[n]) for n in range(4)] + [(w_out_hbm, w_out)]
    fetches = [pltpu.make_async_copy(src, dst, in_sem.at[i]) for i, (src, dst) in enumerate(pairs)]
    for fetch in fetches:
        fetch.start()

    barrier = pltpu.get_barrier_semaphore()
    for other in (sibling, peer(1), peer(2), peer(3)):
        pl.semaphore_signal(barrier, inc=1, device_id=(data, other), device_id_type=MESH)
    pl.semaphore_wait(barrier, 4)

    def remote(src, dst, send, recv, target):
        return pltpu.make_async_remote_copy(src_ref=src, dst_ref=dst, send_sem=send, recv_sem=recv, device_id=(data, target), device_id_type=MESH)

    own = pl.ds(core * STEPS, STEPS)
    for fetch in fetches[:5]:
        fetch.wait()
    for k in range(STEPS):
        hvec[core * STEPS + k] = jnp.full((8, 128), h_ref[k] * (0.5 / SCALE), jnp.float32)
    par_copies = [remote(own_par.at[i], sib_par.at[i], sib_send.at[i], sib_recv.at[i], sibling) for i in range(4)]
    par_copies.append(remote(hvec.at[own], hvec.at[own], sib_send.at[4], sib_recv.at[4], sibling))
    for copy in par_copies:
        copy.start()

    def spread(refs, first):
        for i in range(4):
            full = refs[i][...].astype(jnp.float32)
            full = SCALE * (1.0 + full) if i % 2 == 0 else SCALE * full
            for k in range(STEPS):
                par[first + k, i] = jnp.broadcast_to(full[k:k + 1], (8, HIDDEN))

    def round_rows(c):
        return pl.ds(pl.multiple_of(row0 + c * (DUO * CH), DUO * CH), DUO * CH)

    def stage_x(i, c):
        for t in range(PAIR):
            value = base[c, i] if t == 0 else base[c, i] + loc[t, c, i]
            xb[i, CH * t:CH * t + CH, :] = value.astype(jnp.bfloat16)

    def stage_a(i, tiles=range(4)):
        for n in tiles:
            abuf[i, n] = dot(xb[i], w1[n])

    loc[...] = jnp.zeros_like(loc)
    spread([own_par.at[i] for i in range(4)], core * STEPS)
    for fetch in fetches[5:]:
        fetch.wait()
    base[...] = x_own[...]
    stage_x(0, 0)
    stage_a(0)
    for copy in par_copies:
        copy.wait()
    spread([sib_par.at[i] for i in range(4)], (1 - core) * STEPS)

    guide = guide_ref[0]

    def gelus(i, n):
        lanes = slice(256 * n, 256 * n + 256)
        cond, free = [], []
        for t in range(PAIR):
            wide = [jnp.concatenate([par[t, p, :, lanes]] * (CH // 8), axis=0) for p in range(4)]
            pre = abuf[i, n, CH * t:CH * t + CH, :]
            cond.append(scaled_gelu(pre, wide[0], wide[1]))
            free.append(scaled_gelu(pre, wide[2], wide[3]))
        return jnp.concatenate(cond, axis=0), jnp.concatenate(free, axis=0)

    def stage_f(i, c, event, f_c, f_u):
        total = None
        for t in range(PAIR):
            rows = slice(CH * t, CH * t + CH)
            hk = jnp.concatenate([jnp.concatenate([hvec[t]] * 2, axis=1)] * (CH // 8), axis=0)
            drift = hk * ((1.0 + guide) * f_c[rows] - guide * f_u[rows])
            total = drift if total is None else total + drift
            if t + 1 < PAIR:
                loc[t + 1, c, i] = total
            else:
                tbuf[event, i] = total

    def copy_to(lane, e, src, step):
        return remote(src, rec.at[lane, e], send_sem.at[step - 1, e], recv_sem.at[lane, e], peer(step))

    def send_sum(e):
        @pl.when(chip == 0)
        def _():
            copy_to(0, e, tbuf.at[e], 1).start()

        @pl.when(chip == 2)
        def _():
            copy_to(1, e, tbuf.at[e], 1).start()

    def got(lane, e):
        remote(rec.at[lane, e], rec.at[lane, e], send_sem.at[0, e], recv_sem.at[lane, e], peer(1)).wait_recv()

    def set_base(e, total, last):
        c = lax.rem(e, NCH)
        rows = round_rows(c)
        value = x_own[c]
        if total is not None:
            value = value + total
        if last:
            base_out[rows, :] = value.reshape(DUO * CH, WIDTH)
            remote(base_out.at[rows], base_out.at[rows], out_send.at[1, c], out_recv.at[1, c], sibling).start()
        else:
            base[c] = value

    def relay(e, last):
        @pl.when(chip == 1)
        def _():
            got(0, e)
            below = rec[0, e]
            vbuf[e] = below + tbuf[e]
            copy_to(0, e, vbuf.at[e], 1).start()
            copy_to(0, e, vbuf.at[e], 2).start()
            set_base(e, below, last)

    def take(e, last):
        @pl.when(chip == 2)
        def _():
            got(0, e)
            set_base(e, rec[0, e], last)

        @pl.when(chip == 3)
        def _():
            got(0, e)
            got(1, e)
            set_base(e, rec[0, e] + rec[1, e], last)

    def early_copy(source):
        return remote(tbuf.at[NB - 2], rec_early.at[source], early_send.at[0], early_recv.at[source], peer(2 - source))

    def send_early():
        for source in range(2):
            @pl.when(chip == source)
            def _():
                early_copy(source).start()

    def relay_early():
        e = NB - 2

        @pl.when(chip == 1)
        def _():
            got(0, e)
            below = rec[0, e]
            vbuf[e] = below + tbuf[e]
            copy_to(0, e, vbuf.at[e], 2).start()
            set_base(e, below, True)

        @pl.when(chip == 2)
        def _():
            for source in range(2):
                early_copy(source).wait_recv()
            set_base(e, rec_early[0] + rec_early[1], True)

        @pl.when(chip == 3)
        def _():
            got(0, e)
            got(1, e)
            set_base(e, rec[0, e] + rec[1, e], True)

    def last_copy(source, i, step):
        return remote(tbuf.at[NB - 1, i], rec_last.at[source, i], last_send.at[step - 1, i], last_recv.at[source, i], peer(step))

    def send_last(i):
        for source in range(3):
            @pl.when(chip == source)
            def _():
                for step in range(3 - source, 0, -1):
                    last_copy(source, i, step).start()

    def half_rows(i):
        return pl.ds(pl.multiple_of(row0 + ((NCH - 1) * DUO + i) * CH, CH), CH)

    def base_copy(i):
        return remote(base_out.at[half_rows(i)], base_out.at[half_rows(i)], base_send.at[i], base_recv.at[i], sibling)

    def take_last(i):
        for mine in range(4):
            @pl.when(chip == mine)
            def _():
                value = x_own[NCH - 1, i]
                for source in range(mine):
                    last_copy(source, i, 1).wait_recv()
                    value = value + rec_last[source, i]
                base_out[half_rows(i), :] = value
                base_copy(i).start()

    def send_local(e):
        c = lax.rem(e, NCH)
        for k in range(STEPS):
            loc_out[k, core * NCH + c] = loc[core * STEPS + k, c]
        local_copy(c).start()

    def local_copy(c):
        return remote(loc.at[pl.ds((1 - core) * STEPS, STEPS), c], loc_out.at[:, core * NCH + c], out_send.at[0, c], out_recv.at[0, c], sibling)

    def one_block(i, c, c_after, event):
        follow = (i + 1) % DUO
        stage_x(follow, c_after)
        f_c = f_u = None
        for n in range(4):
            weight = w_out[256 * n:256 * n + 256, :]
            cond, free = gelus(i, n)
            part_c, part_u = dot(cond, weight), dot(free, weight)
            f_c = part_c if n == 0 else f_c + part_c
            f_u = part_u if n == 0 else f_u + part_u
            if n in AHEAD[i]:
                stage_a(follow, AHEAD[i][n])
        stage_f(i, c, event, f_c, f_u)

    def one_round(r, carry):
        c = lax.rem(r, NCH)

        @pl.when(r >= 1)
        def _():
            send_sum(r - 1)

        @pl.when((r >= PASS) & (r < PASS + NB - NCH))
        def _():
            relay(r - PASS, False)

        @pl.when(r >= PASS + NB - NCH)
        def _():
            relay(r - PASS, True)

        @pl.when(r >= NEED)
        def _():
            take(r - NEED, False)

        @pl.when(r >= NB - NCH + 1)
        def _():
            send_local(r - 1)

        one_block(0, c, c, r)
        one_block(1, c, lax.rem(r + 1, NCH), r)
        return carry

    lax.fori_loop(0, NB - 1, one_round, 0)
    send_sum(NB - 2)
    send_early()
    relay(NB - 1 - PASS, True)
    take(NB - 1 - NEED, True)
    send_local(NB - 2)

    @pl.when(chip == 0)
    def _():
        for c in range(NCH - 1):
            set_base(c, None, True)

    one_block(0, NCH - 1, NCH - 1, NB - 1)
    send_last(0)
    one_block(1, NCH - 1, 0, NB - 1)
    send_last(1)
    send_local(NB - 1)
    for e in range(NB - NEED, NB - 2):
        take(e, True)
    relay_early()
    take_last(0)
    take_last(1)

    def drain(e, carry):
        @pl.when((chip == 0) | (chip == 2))
        def _():
            copy_to(0, e, tbuf.at[e], 1).wait_send()

        @pl.when(chip == 1)
        def _():
            copy_to(0, e, vbuf.at[e], 1).wait_send()
            copy_to(0, e, vbuf.at[e], 2).wait_send()
        return carry

    def finish_local(c, carry):
        local_copy(c).wait()
        return carry

    def finish_base(c, carry):
        rows = round_rows(c)
        remote(base_out.at[rows], base_out.at[rows], out_send.at[1, c], out_recv.at[1, c], sibling).wait()
        return carry

    lax.fori_loop(0, NB - 2, drain, 0)

    @pl.when((chip == 0) | (chip == 2))
    def _():
        copy_to(0, NB - 2, tbuf.at[NB - 2], 1).wait_send()

    @pl.when(chip == 1)
    def _():
        copy_to(0, NB - 2, vbuf.at[NB - 2], 2).wait_send()

    @pl.when(chip < 2)
    def _():
        early_copy(0).wait_send()

    for source in range(3):
        @pl.when(chip == source)
        def _():
            for i in range(DUO):
                for step in range(1, 4 - source):
                    last_copy(source, i, step).wait_send()

    lax.fori_loop(0, NCH, finish_local, 0)
    lax.fori_loop(0, NCH - 1, finish_base, 0)
    base_copy(0).wait()
    base_copy(1).wait()


def finish(loc_ref, base_ref, out_hbm, stage, sem):
    pieces = []
    for piece in range(PIECES):
        rows = pl.ds(piece * (2 * OWN // PIECES), 2 * OWN // PIECES)
        for k in range(STEPS):
            stage[k, rows, :] = base_ref[rows, :] + loc_ref[k, rows, :]
        pieces.append(pltpu.make_async_copy(stage.at[:, rows], out_hbm.at[:, rows], sem.at[piece]))
        pieces[-1].start()
    for copy in pieces:
        copy.wait()


def solution(mesh):
    vmem = pl.BlockSpec(memory_space=pltpu.VMEM)
    smem = pl.BlockSpec(memory_space=pltpu.SMEM)
    hbm = pl.BlockSpec(memory_space=pltpu.HBM)
    dma = pltpu.SemaphoreType.DMA

    def local(x_init, w_in, w_out, gamma_c, beta_c, gamma_u, beta_u, step_h, guide_w):
        samples, tokens, width = x_init.shape
        rows = samples * tokens
        loc, base = pl.pallas_call(
            kernel,
            out_shape=(jax.ShapeDtypeStruct((STEPS, 2 * NCH, DUO, CH, width), jnp.float32), jax.ShapeDtypeStruct((rows, width), jnp.float32)),
            in_specs=[hbm] * 8 + [smem],
            out_specs=(vmem, vmem),
            scratch_shapes=[
                pltpu.SMEM((STEPS,), jnp.float32),
                pltpu.VMEM((NCH, DUO, CH, WIDTH), jnp.float32),
                pltpu.VMEM((HIDDEN, WIDTH), jnp.bfloat16),
                pltpu.VMEM((PAIR, NCH, DUO, CH, WIDTH), jnp.float32),
                pltpu.VMEM((NCH, DUO, CH, WIDTH), jnp.float32),
                pltpu.VMEM((PAIR, 4, 8, HIDDEN), jnp.float32),
                pltpu.VMEM((PAIR, 8, 128), jnp.float32),
                pltpu.VMEM((4, STEPS, HIDDEN), jnp.bfloat16),
                pltpu.VMEM((4, STEPS, HIDDEN), jnp.bfloat16),
                pltpu.VMEM((4, WIDTH, WIDTH), jnp.bfloat16),
                pltpu.VMEM((DUO, ROWS, WIDTH), jnp.bfloat16),
                pltpu.VMEM((DUO, 4, ROWS, WIDTH), jnp.float32),
                pltpu.VMEM((NB, DUO, CH, WIDTH), jnp.float32),
                pltpu.VMEM((NB, DUO, CH, WIDTH), jnp.float32),
                pltpu.VMEM((2, NB, DUO, CH, WIDTH), jnp.float32),
                pltpu.VMEM((2, DUO, CH, WIDTH), jnp.float32),
                pltpu.VMEM((3, DUO, CH, WIDTH), jnp.float32),
                dma((11,)), dma((5,)), dma((5,)), dma((2, NB - 1)), dma((2, NB - 1)), dma((2, NCH)), dma((2, NCH)),
                dma((3, DUO)), dma((3, DUO)), dma((DUO,)), dma((DUO,)), dma((1,)), dma((2,)),
            ],
            compiler_params=pltpu.CompilerParams(collective_id=0, has_side_effects=True, vmem_limit_bytes=48 * 2 ** 20),
            name="picard",
        )(*(pltpu.with_memory_space_constraint(value, pltpu.HBM) for value in (x_init.reshape(2, NCH, DUO, CH, width), w_in, w_out, gamma_c, beta_c, gamma_u, beta_u, step_h)), guide_w)
        out = pl.pallas_call(
            finish,
            out_shape=jax.ShapeDtypeStruct((STEPS, rows, width), jnp.float32),
            in_specs=[vmem] * 2,
            out_specs=hbm,
            scratch_shapes=[pltpu.VMEM((STEPS, rows, width), jnp.float32), dma((PIECES,))],
            compiler_params=pltpu.CompilerParams(vmem_limit_bytes=8 * 2 ** 20),
            name="finish",
        )(loc.reshape(STEPS, rows, width), base)
        return out.reshape(STEPS, samples, tokens, width)

    return jax.shard_map(local, mesh=mesh, in_specs=(P("data", None, None), P(None, None), P(None, None), P("time", None), P("time", None), P("time", None), P("time", None), P("time"), P(None)), out_specs=P("time", "data", None, None), check_vma=False)
```

```python
import functools
import math

import jax
import jax.numpy as jnp
from jax import lax
from jax.experimental import pallas as pl
from jax.experimental.pallas import tpu as pltpu
from jax.sharding import PartitionSpec as P

NUM_SWEEPS = 4
ROOT = math.sqrt(2.0 / math.pi)
SCALE = (ROOT * 0.044715) ** (1.0 / 3.0)
LIN = ROOT / SCALE
CH = 32
DUO = 2
NCH = 4
NB = NUM_SWEEPS * NCH
OWN = CH * DUO * NCH
STEPS = 6
PAIR = 2 * STEPS
ROWS = PAIR * CH
WIDTH = 256
PIECES = 8
HIDDEN = 1024
NEED = 3
PASS = 2
AHEAD = ({1: (0,), 2: (1, 2), 3: (3,)}, {1: (0,), 2: (1, 2), 3: (3,)})
LATE = 2
MESH = pl.DeviceIdType.MESH

dot = functools.partial(jnp.dot, preferred_element_type=jnp.float32)


def scaled_gelu(pre, gain, shift):
    y = pre * gain + shift
    return (y * (1.0 + jnp.tanh(y * (y * y + LIN)))).astype(jnp.bfloat16)


def kernel(x_hbm, w_in, w_out_hbm, gamma_c, beta_c, gamma_u, beta_u, h_hbm, guide_ref, loc_out, base_out, h_ref, x_own, w_out, loc, base, par, hvec, own_par,
           sib_par, w1, xb, abuf, tbuf, vbuf, rec, rec_early, rec_last, vlast, in_sem, sib_send, sib_recv, send_sem, recv_sem, out_send, out_recv, last_send, last_recv,
           base_send, base_recv, early_send, early_recv):
    time = lax.axis_index("time")
    data = lax.axis_index("data")
    core = lax.rem(time, 2)
    chip = lax.div(time, 2)
    sibling = time + 1 - 2 * core
    row0 = pl.multiple_of(core * OWN, OWN)

    def peer(step):
        return lax.rem(time + 2 * step, 8)

    raw = [gamma_c, beta_c, gamma_u, beta_u]
    pairs = [(raw[i], own_par.at[i]) for i in range(4)] + [(h_hbm, h_ref), (x_hbm.at[core], x_own)]
    pairs += [(w_in.at[:, pl.ds(256 * n, 256)], w1.at[n]) for n in range(4)] + [(w_out_hbm, w_out)]
    fetches = [pltpu.make_async_copy(src, dst, in_sem.at[i]) for i, (src, dst) in enumerate(pairs)]
    for fetch in fetches:
        fetch.start()

    barrier = pltpu.get_barrier_semaphore()
    for other in (sibling, peer(1), peer(2), peer(3)):
        pl.semaphore_signal(barrier, inc=1, device_id=(data, other), device_id_type=MESH)
    pl.semaphore_wait(barrier, 4)

    def remote(src, dst, send, recv, target):
        return pltpu.make_async_remote_copy(src_ref=src, dst_ref=dst, send_sem=send, recv_sem=recv, device_id=(data, target), device_id_type=MESH)

    own = pl.ds(core * STEPS, STEPS)
    for fetch in fetches[:5]:
        fetch.wait()
    for k in range(STEPS):
        hvec[core * STEPS + k] = jnp.full((8, 128), h_ref[k] * (0.5 / SCALE), jnp.float32)
    par_copies = [remote(own_par.at[i], sib_par.at[i], sib_send.at[i], sib_recv.at[i], sibling) for i in range(4)]
    par_copies.append(remote(hvec.at[own], hvec.at[own], sib_send.at[4], sib_recv.at[4], sibling))
    for copy in par_copies:
        copy.start()

    def spread(refs, first):
        for i in range(4):
            full = refs[i][...].astype(jnp.float32)
            full = SCALE * (1.0 + full) if i % 2 == 0 else SCALE * full
            for k in range(STEPS):
                par[first + k, i] = jnp.broadcast_to(full[k:k + 1], (8, HIDDEN))

    def round_rows(c):
        return pl.ds(pl.multiple_of(row0 + c * (DUO * CH), DUO * CH), DUO * CH)

    def stage_x(i, c):
        for t in range(PAIR):
            value = base[c, i] if t == 0 else base[c, i] + loc[t, c, i]
            xb[i, CH * t:CH * t + CH, :] = value.astype(jnp.bfloat16)

    def stage_a(i, tiles=range(4)):
        for n in tiles:
            abuf[i, n] = dot(xb[i], w1[n])

    loc[...] = jnp.zeros_like(loc)
    spread([own_par.at[i] for i in range(4)], core * STEPS)
    for fetch in fetches[5:]:
        fetch.wait()
    base[...] = x_own[...]
    stage_x(0, 0)
    stage_a(0)
    for copy in par_copies:
        copy.wait()
    spread([sib_par.at[i] for i in range(4)], (1 - core) * STEPS)

    guide = guide_ref[0]

    def gelus(i, n):
        lanes = slice(256 * n, 256 * n + 256)
        cond, free = [], []
        for t in range(PAIR):
            wide = [jnp.concatenate([par[t, p, :, lanes]] * (CH // 8), axis=0) for p in range(4)]
            pre = abuf[i, n, CH * t:CH * t + CH, :]
            cond.append(scaled_gelu(pre, wide[0], wide[1]))
            free.append(scaled_gelu(pre, wide[2], wide[3]))
        return jnp.concatenate(cond, axis=0), jnp.concatenate(free, axis=0)

    def stage_f(i, c, event, f_c, f_u):
        total = None
        for t in range(PAIR):
            rows = slice(CH * t, CH * t + CH)
            hk = jnp.concatenate([jnp.concatenate([hvec[t]] * 2, axis=1)] * (CH // 8), axis=0)
            drift = hk * ((1.0 + guide) * f_c[rows] - guide * f_u[rows])
            total = drift if total is None else total + drift
            if t + 1 < PAIR:
                loc[t + 1, c, i] = total
            else:
                tbuf[event, i] = total

    def copy_to(lane, e, src, step):
        return remote(src, rec.at[lane, e], send_sem.at[step - 1, e], recv_sem.at[lane, e], peer(step))

    def send_sum(e):
        @pl.when(chip == 0)
        def _():
            copy_to(0, e, tbuf.at[e], 1).start()

        @pl.when(chip == 2)
        def _():
            copy_to(1, e, tbuf.at[e], 1).start()

    def got(lane, e):
        remote(rec.at[lane, e], rec.at[lane, e], send_sem.at[0, e], recv_sem.at[lane, e], peer(1)).wait_recv()

    def set_base(e, total, last):
        c = lax.rem(e, NCH)
        rows = round_rows(c)
        value = x_own[c]
        if total is not None:
            value = value + total
        if last:
            base_out[rows, :] = value.reshape(DUO * CH, WIDTH)
            remote(base_out.at[rows], base_out.at[rows], out_send.at[1, c], out_recv.at[1, c], sibling).start()
        else:
            base[c] = value

    def relay(e, last):
        @pl.when(chip == 1)
        def _():
            got(0, e)
            below = rec[0, e]
            vbuf[e] = below + tbuf[e]
            copy_to(0, e, vbuf.at[e], 1).start()
            copy_to(0, e, vbuf.at[e], 2).start()
            set_base(e, below, last)

    def take(e, last):
        @pl.when(chip == 2)
        def _():
            got(0, e)
            set_base(e, rec[0, e], last)

        @pl.when(chip == 3)
        def _():
            got(0, e)
            got(1, e)
            set_base(e, rec[0, e] + rec[1, e], last)

    def early_copy(source):
        return remote(tbuf.at[NB - 2], rec_early.at[source], early_send.at[0], early_recv.at[source], peer(2 - source))

    def send_early():
        for source in range(2):
            @pl.when(chip == source)
            def _():
                early_copy(source).start()

    def relay_early():
        e = NB - 2

        @pl.when(chip == 1)
        def _():
            got(0, e)
            below = rec[0, e]
            vbuf[e] = below + tbuf[e]
            copy_to(0, e, vbuf.at[e], 2).start()
            set_base(e, below, True)

    def take_early():
        e = NB - 2

        @pl.when(chip == 2)
        def _():
            for source in range(2):
                early_copy(source).wait_recv()
            set_base(e, rec_early[0] + rec_early[1], True)

        @pl.when(chip == 3)
        def _():
            got(0, e)
            got(1, e)
            set_base(e, rec[0, e] + rec[1, e], True)

    def last_copy(source, i, step):
        return remote(tbuf.at[NB - 1, i], rec_last.at[source, i], last_send.at[step - 1, i], last_recv.at[source, i], peer(step))

    def send_last(i):
        for source in (0, 2):
            @pl.when(chip == source)
            def _():
                last_copy(source, i, 1).start()

    def vlast_copy(i, step):
        return remote(vlast.at[i], rec_last.at[1, i], last_send.at[step - 1, i], last_recv.at[1, i], peer(step))

    def relay_last(i):
        @pl.when(chip == 1)
        def _():
            last_copy(0, i, 1).wait_recv()
            vlast[i] = rec_last[0, i] + tbuf[NB - 1, i]
            for step in (1, 2):
                vlast_copy(i, step).start()

    def half_rows(i):
        return pl.ds(pl.multiple_of(row0 + ((NCH - 1) * DUO + i) * CH, CH), CH)

    def base_copy(i):
        return remote(base_out.at[half_rows(i)], base_out.at[half_rows(i)], base_send.at[i], base_recv.at[i], sibling)

    def take_last(i):
        for mine in range(4):
            @pl.when(chip == mine)
            def _():
                value = x_own[NCH - 1, i]
                for source in range(1, mine):
                    last_copy(source, i, 1).wait_recv()
                    value = value + rec_last[source, i]
                if mine == 1:
                    value = value + rec_last[0, i]
                base_out[half_rows(i), :] = value
                base_copy(i).start()

    def send_local(e):
        c = lax.rem(e, NCH)
        for k in range(STEPS):
            loc_out[k, core * NCH + c] = loc[core * STEPS + k, c]
        local_copy(c).start()

    def local_copy(c):
        return remote(loc.at[pl.ds((1 - core) * STEPS, STEPS), c], loc_out.at[:, core * NCH + c], out_send.at[0, c], out_recv.at[0, c], sibling)

    def one_block(i, c, c_after, event):
        follow = (i + 1) % DUO
        stage_x(follow, c_after)
        f_c = f_u = None
        for n in range(4):
            weight = w_out[256 * n:256 * n + 256, :]
            cond, free = gelus(i, n)
            part_c, part_u = dot(cond, weight), dot(free, weight)
            f_c = part_c if n == 0 else f_c + part_c
            f_u = part_u if n == 0 else f_u + part_u
            if n in AHEAD[i]:
                stage_a(follow, AHEAD[i][n])
        stage_f(i, c, event, f_c, f_u)

    def one_round(r, carry):
        c = lax.rem(r, NCH)

        @pl.when(r >= 1)
        def _():
            send_sum(r - 1)

        @pl.when((r >= PASS) & (r < PASS + NB - NCH))
        def _():
            relay(r - PASS, False)

        @pl.when(r >= PASS + NB - NCH)
        def _():
            relay(r - PASS, True)

        @pl.when(r >= NEED)
        def _():
            take(r - NEED, False)

        @pl.when(r >= NB - NCH + 1)
        def _():
            send_local(r - 1)

        one_block(0, c, c, r)
        one_block(1, c, lax.rem(r + 1, NCH), r)
        return carry

    lax.fori_loop(0, NB - 1, one_round, 0)
    send_sum(NB - 2)
    send_early()
    relay(NB - 1 - PASS, True)
    take(NB - 1 - NEED, True)
    send_local(NB - 2)

    @pl.when(chip == 0)
    def _():
        for c in range(NCH - 1):
            set_base(c, None, True)

    one_block(0, NCH - 1, NCH - 1, NB - 1)
    send_last(0)
    one_block(1, NCH - 1, 0, NB - 1)
    send_last(1)
    send_local(NB - 1)

    def drain(e, carry):
        @pl.when((chip == 0) | (chip == 2))
        def _():
            copy_to(0, e, tbuf.at[e], 1).wait_send()

        @pl.when(chip == 1)
        def _():
            copy_to(0, e, vbuf.at[e], 1).wait_send()
            copy_to(0, e, vbuf.at[e], 2).wait_send()
        return carry

    def finish_local(c, carry):
        local_copy(c).wait()
        return carry

    def finish_base(c, carry):
        rows = round_rows(c)
        remote(base_out.at[rows], base_out.at[rows], out_send.at[1, c], out_recv.at[1, c], sibling).wait()
        return carry

    relay_early()
    relay_last(0)
    relay_last(1)
    lax.fori_loop(0, NB - 1 - LATE, drain, 0)
    lax.fori_loop(0, NCH - 1, finish_local, 0)
    for e in range(NB - NEED, NB - 2):
        take(e, True)
    take_early()
    take_last(0)
    take_last(1)

    for e in range(NB - 1 - LATE, NB - 2):
        drain(e, 0)

    @pl.when((chip == 0) | (chip == 2))
    def _():
        copy_to(0, NB - 2, tbuf.at[NB - 2], 1).wait_send()

    @pl.when(chip == 1)
    def _():
        copy_to(0, NB - 2, vbuf.at[NB - 2], 2).wait_send()

    @pl.when(chip < 2)
    def _():
        early_copy(0).wait_send()

    for i in range(DUO):
        @pl.when((chip == 0) | (chip == 2))
        def _():
            last_copy(0, i, 1).wait_send()

        @pl.when(chip == 1)
        def _():
            for step in (1, 2):
                vlast_copy(i, step).wait_send()

    local_copy(NCH - 1).wait()
    for c in range(NCH - 1):
        finish_base(c, 0)
    base_copy(0).wait()
    base_copy(1).wait()


def finish(loc_ref, base_ref, out_hbm, stage, sem):
    pieces = []
    for piece in range(PIECES):
        rows = pl.ds(piece * (2 * OWN // PIECES), 2 * OWN // PIECES)
        for k in range(STEPS):
            stage[k, rows, :] = base_ref[rows, :] + loc_ref[k, rows, :]
        pieces.append(pltpu.make_async_copy(stage.at[:, rows], out_hbm.at[:, rows], sem.at[piece]))
        pieces[-1].start()
    for copy in pieces:
        copy.wait()


def solution(mesh):
    vmem = pl.BlockSpec(memory_space=pltpu.VMEM)
    smem = pl.BlockSpec(memory_space=pltpu.SMEM)
    hbm = pl.BlockSpec(memory_space=pltpu.HBM)
    dma = pltpu.SemaphoreType.DMA

    def local(x_init, w_in, w_out, gamma_c, beta_c, gamma_u, beta_u, step_h, guide_w):
        samples, tokens, width = x_init.shape
        rows = samples * tokens
        loc, base = pl.pallas_call(
            kernel,
            out_shape=(jax.ShapeDtypeStruct((STEPS, 2 * NCH, DUO, CH, width), jnp.float32), jax.ShapeDtypeStruct((rows, width), jnp.float32)),
            in_specs=[hbm] * 8 + [smem],
            out_specs=(vmem, vmem),
            scratch_shapes=[
                pltpu.SMEM((STEPS,), jnp.float32),
                pltpu.VMEM((NCH, DUO, CH, WIDTH), jnp.float32),
                pltpu.VMEM((HIDDEN, WIDTH), jnp.bfloat16),
                pltpu.VMEM((PAIR, NCH, DUO, CH, WIDTH), jnp.float32),
                pltpu.VMEM((NCH, DUO, CH, WIDTH), jnp.float32),
                pltpu.VMEM((PAIR, 4, 8, HIDDEN), jnp.float32),
                pltpu.VMEM((PAIR, 8, 128), jnp.float32),
                pltpu.VMEM((4, STEPS, HIDDEN), jnp.bfloat16),
                pltpu.VMEM((4, STEPS, HIDDEN), jnp.bfloat16),
                pltpu.VMEM((4, WIDTH, WIDTH), jnp.bfloat16),
                pltpu.VMEM((DUO, ROWS, WIDTH), jnp.bfloat16),
                pltpu.VMEM((DUO, 4, ROWS, WIDTH), jnp.float32),
                pltpu.VMEM((NB, DUO, CH, WIDTH), jnp.float32),
                pltpu.VMEM((NB, DUO, CH, WIDTH), jnp.float32),
                pltpu.VMEM((2, NB, DUO, CH, WIDTH), jnp.float32),
                pltpu.VMEM((2, DUO, CH, WIDTH), jnp.float32),
                pltpu.VMEM((3, DUO, CH, WIDTH), jnp.float32),
                pltpu.VMEM((DUO, CH, WIDTH), jnp.float32),
                dma((11,)), dma((5,)), dma((5,)), dma((2, NB - 1)), dma((2, NB - 1)), dma((2, NCH)), dma((2, NCH)),
                dma((3, DUO)), dma((3, DUO)), dma((DUO,)), dma((DUO,)), dma((1,)), dma((2,)),
            ],
            compiler_params=pltpu.CompilerParams(collective_id=0, has_side_effects=True, vmem_limit_bytes=48 * 2 ** 20),
            name="picard",
        )(*(pltpu.with_memory_space_constraint(value, pltpu.HBM) for value in (x_init.reshape(2, NCH, DUO, CH, width), w_in, w_out, gamma_c, beta_c, gamma_u, beta_u, step_h)), guide_w)
        out = pl.pallas_call(
            finish,
            out_shape=jax.ShapeDtypeStruct((STEPS, rows, width), jnp.float32),
            in_specs=[vmem] * 2,
            out_specs=hbm,
            scratch_shapes=[pltpu.VMEM((STEPS, rows, width), jnp.float32), dma((PIECES,))],
            compiler_params=pltpu.CompilerParams(vmem_limit_bytes=8 * 2 ** 20),
            name="finish",
        )(loc.reshape(STEPS, rows, width), base)
        return out.reshape(STEPS, samples, tokens, width)

    return jax.shard_map(local, mesh=mesh, in_specs=(P("data", None, None), P(None, None), P(None, None), P("time", None), P("time", None), P("time", None), P("time", None), P("time"), P(None)), out_specs=P("time", "data", None, None), check_vma=False)
```

```python
import functools
import math

import jax
import jax.numpy as jnp
from jax import lax
from jax.experimental import pallas as pl
from jax.experimental.pallas import tpu as pltpu
from jax.sharding import PartitionSpec as P

NUM_SWEEPS = 4
ROOT = math.sqrt(2.0 / math.pi)
SCALE = (ROOT * 0.044715) ** (1.0 / 3.0)
LIN = ROOT / SCALE
CH = 32
DUO = 2
NCH = 4
NB = NUM_SWEEPS * NCH
OWN = CH * DUO * NCH
STEPS = 6
PAIR = 2 * STEPS
ROWS = PAIR * CH
WIDTH = 256
PIECES = 16
HIDDEN = 1024
NEED = 3
PASS = 2
AHEAD = ({1: (0,), 2: (1, 2), 3: (3,)}, {1: (0,), 2: (1, 2), 3: (3,)})
LATE = 2
MESH = pl.DeviceIdType.MESH

dot = functools.partial(jnp.dot, preferred_element_type=jnp.float32)


def scaled_gelu(pre, gain, shift):
    y = pre * gain + shift
    return (y * (1.0 + jnp.tanh(y * (y * y + LIN)))).astype(jnp.bfloat16)


def kernel(x_hbm, w_in, w_out_hbm, gamma_c, beta_c, gamma_u, beta_u, h_hbm, guide_ref, loc_out, base_out, h_ref, x_own, w_out, loc, base, par, hvec, own_par,
           sib_par, w1, xb, abuf, tbuf, vbuf, rec, rec_early, rec_last, vlast, in_sem, sib_send, sib_recv, send_sem, recv_sem, out_send, out_recv, last_send, last_recv,
           base_send, base_recv, early_send, early_recv):
    time = lax.axis_index("time")
    data = lax.axis_index("data")
    core = lax.rem(time, 2)
    chip = lax.div(time, 2)
    sibling = time + 1 - 2 * core
    row0 = pl.multiple_of(core * OWN, OWN)

    def peer(step):
        return lax.rem(time + 2 * step, 8)

    raw = [gamma_c, beta_c, gamma_u, beta_u]
    pairs = [(raw[i], own_par.at[i]) for i in range(4)] + [(h_hbm, h_ref), (x_hbm.at[core], x_own)]
    pairs += [(w_in.at[:, pl.ds(256 * n, 256)], w1.at[n]) for n in range(4)] + [(w_out_hbm, w_out)]
    fetches = [pltpu.make_async_copy(src, dst, in_sem.at[i]) for i, (src, dst) in enumerate(pairs)]
    for fetch in fetches:
        fetch.start()

    barrier = pltpu.get_barrier_semaphore()
    for other in (sibling, peer(1), peer(2), peer(3)):
        pl.semaphore_signal(barrier, inc=1, device_id=(data, other), device_id_type=MESH)
    pl.semaphore_wait(barrier, 4)

    def remote(src, dst, send, recv, target):
        return pltpu.make_async_remote_copy(src_ref=src, dst_ref=dst, send_sem=send, recv_sem=recv, device_id=(data, target), device_id_type=MESH)

    own = pl.ds(core * STEPS, STEPS)
    for fetch in fetches[:5]:
        fetch.wait()
    for k in range(STEPS):
        hvec[core * STEPS + k] = jnp.full((8, 128), h_ref[k] * (0.5 / SCALE), jnp.float32)
    par_copies = [remote(own_par.at[i], sib_par.at[i], sib_send.at[i], sib_recv.at[i], sibling) for i in range(4)]
    par_copies.append(remote(hvec.at[own], hvec.at[own], sib_send.at[4], sib_recv.at[4], sibling))
    for copy in par_copies:
        copy.start()

    def spread(refs, first):
        for i in range(4):
            full = refs[i][...].astype(jnp.float32)
            full = SCALE * (1.0 + full) if i % 2 == 0 else SCALE * full
            for k in range(STEPS):
                par[first + k, i] = jnp.broadcast_to(full[k:k + 1], (8, HIDDEN))

    def round_rows(c):
        return pl.ds(pl.multiple_of(row0 + c * (DUO * CH), DUO * CH), DUO * CH)

    def stage_x(i, c):
        for t in range(PAIR):
            value = base[c, i] if t == 0 else base[c, i] + loc[t, c, i]
            xb[i, CH * t:CH * t + CH, :] = value.astype(jnp.bfloat16)

    def stage_a(i, tiles=range(4)):
        for n in tiles:
            abuf[i, n] = dot(xb[i], w1[n])

    loc[...] = jnp.zeros_like(loc)
    spread([own_par.at[i] for i in range(4)], core * STEPS)
    for fetch in fetches[5:]:
        fetch.wait()
    base[...] = x_own[...]
    stage_x(0, 0)
    stage_a(0)
    for copy in par_copies:
        copy.wait()
    spread([sib_par.at[i] for i in range(4)], (1 - core) * STEPS)

    guide = guide_ref[0]

    def gelus(i, n):
        lanes = slice(256 * n, 256 * n + 256)
        cond, free = [], []
        for t in range(PAIR):
            wide = [jnp.concatenate([par[t, p, :, lanes]] * (CH // 8), axis=0) for p in range(4)]
            pre = abuf[i, n, CH * t:CH * t + CH, :]
            cond.append(scaled_gelu(pre, wide[0], wide[1]))
            free.append(scaled_gelu(pre, wide[2], wide[3]))
        return jnp.concatenate(cond, axis=0), jnp.concatenate(free, axis=0)

    def stage_f(i, c, event, f_c, f_u):
        total = None
        for t in range(PAIR):
            rows = slice(CH * t, CH * t + CH)
            hk = jnp.concatenate([jnp.concatenate([hvec[t]] * 2, axis=1)] * (CH // 8), axis=0)
            drift = hk * ((1.0 + guide) * f_c[rows] - guide * f_u[rows])
            total = drift if total is None else total + drift
            if t + 1 < PAIR:
                loc[t + 1, c, i] = total
            else:
                tbuf[event, i] = total

    def copy_to(lane, e, src, step):
        return remote(src, rec.at[lane, e], send_sem.at[step - 1, e], recv_sem.at[lane, e], peer(step))

    def send_sum(e):
        @pl.when(chip == 0)
        def _():
            copy_to(0, e, tbuf.at[e], 1).start()

        @pl.when(chip == 2)
        def _():
            copy_to(1, e, tbuf.at[e], 1).start()

    def got(lane, e):
        remote(rec.at[lane, e], rec.at[lane, e], send_sem.at[0, e], recv_sem.at[lane, e], peer(1)).wait_recv()

    def set_base(e, total, last):
        c = lax.rem(e, NCH)
        rows = round_rows(c)
        value = x_own[c]
        if total is not None:
            value = value + total
        if last:
            base_out[rows, :] = value.reshape(DUO * CH, WIDTH)
            remote(base_out.at[rows], base_out.at[rows], out_send.at[1, c], out_recv.at[1, c], sibling).start()
        else:
            base[c] = value

    def relay(e, last):
        @pl.when(chip == 1)
        def _():
            got(0, e)
            below = rec[0, e]
            vbuf[e] = below + tbuf[e]
            copy_to(0, e, vbuf.at[e], 1).start()
            copy_to(0, e, vbuf.at[e], 2).start()
            set_base(e, below, last)

    def take(e, last):
        @pl.when(chip == 2)
        def _():
            got(0, e)
            set_base(e, rec[0, e], last)

        @pl.when(chip == 3)
        def _():
            got(0, e)
            got(1, e)
            set_base(e, rec[0, e] + rec[1, e], last)

    def early_copy(source):
        return remote(tbuf.at[NB - 2], rec_early.at[source], early_send.at[0], early_recv.at[source], peer(2 - source))

    def send_early():
        for source in range(2):
            @pl.when(chip == source)
            def _():
                early_copy(source).start()

    def relay_early():
        e = NB - 2

        @pl.when(chip == 1)
        def _():
            got(0, e)
            below = rec[0, e]
            vbuf[e] = below + tbuf[e]
            copy_to(0, e, vbuf.at[e], 2).start()
            set_base(e, below, True)

    def take_early():
        e = NB - 2

        @pl.when(chip == 2)
        def _():
            for source in range(2):
                early_copy(source).wait_recv()
            set_base(e, rec_early[0] + rec_early[1], True)

        @pl.when(chip == 3)
        def _():
            got(0, e)
            got(1, e)
            set_base(e, rec[0, e] + rec[1, e], True)

    def last_copy(source, i, step):
        return remote(tbuf.at[NB - 1, i], rec_last.at[source, i], last_send.at[step - 1, i], last_recv.at[source, i], peer(step))

    def send_last(i):
        for source in (0, 2):
            @pl.when(chip == source)
            def _():
                last_copy(source, i, 1).start()

    def vlast_copy(i, step):
        return remote(vlast.at[i], rec_last.at[1, i], last_send.at[step - 1, i], last_recv.at[1, i], peer(step))

    def relay_last(i):
        @pl.when(chip == 1)
        def _():
            last_copy(0, i, 1).wait_recv()
            vlast[i] = rec_last[0, i] + tbuf[NB - 1, i]
            for step in (1, 2):
                vlast_copy(i, step).start()

    def half_rows(i):
        return pl.ds(pl.multiple_of(row0 + ((NCH - 1) * DUO + i) * CH, CH), CH)

    def base_copy(i):
        return remote(base_out.at[half_rows(i)], base_out.at[half_rows(i)], base_send.at[i], base_recv.at[i], sibling)

    def take_last(i):
        for mine in range(4):
            @pl.when(chip == mine)
            def _():
                value = x_own[NCH - 1, i]
                for source in range(1, mine):
                    last_copy(source, i, 1).wait_recv()
                    value = value + rec_last[source, i]
                if mine == 1:
                    value = value + rec_last[0, i]
                base_out[half_rows(i), :] = value
                base_copy(i).start()

    def send_local(e):
        c = lax.rem(e, NCH)
        for k in range(STEPS):
            loc_out[k, core * NCH + c] = loc[core * STEPS + k, c]
        local_copy(c).start()

    def local_copy(c):
        return remote(loc.at[pl.ds((1 - core) * STEPS, STEPS), c], loc_out.at[:, core * NCH + c], out_send.at[0, c], out_recv.at[0, c], sibling)

    def one_block(i, c, c_after, event):
        follow = (i + 1) % DUO
        stage_x(follow, c_after)
        f_c = f_u = None
        for n in range(4):
            weight = w_out[256 * n:256 * n + 256, :]
            cond, free = gelus(i, n)
            part_c, part_u = dot(cond, weight), dot(free, weight)
            f_c = part_c if n == 0 else f_c + part_c
            f_u = part_u if n == 0 else f_u + part_u
            if n in AHEAD[i]:
                stage_a(follow, AHEAD[i][n])
        stage_f(i, c, event, f_c, f_u)

    def one_round(r, carry):
        c = lax.rem(r, NCH)

        @pl.when(r >= 1)
        def _():
            send_sum(r - 1)

        @pl.when((r >= PASS) & (r < PASS + NB - NCH))
        def _():
            relay(r - PASS, False)

        @pl.when(r >= PASS + NB - NCH)
        def _():
            relay(r - PASS, True)

        @pl.when(r >= NEED)
        def _():
            take(r - NEED, False)

        @pl.when(r >= NB - NCH + 1)
        def _():
            send_local(r - 1)

        one_block(0, c, c, r)
        one_block(1, c, lax.rem(r + 1, NCH), r)
        return carry

    lax.fori_loop(0, NB - 1, one_round, 0)
    send_sum(NB - 2)
    send_early()
    relay(NB - 1 - PASS, True)
    take(NB - 1 - NEED, True)
    send_local(NB - 2)

    @pl.when(chip == 0)
    def _():
        for c in range(NCH - 1):
            set_base(c, None, True)

    one_block(0, NCH - 1, NCH - 1, NB - 1)
    send_last(0)
    one_block(1, NCH - 1, 0, NB - 1)
    send_last(1)
    send_local(NB - 1)

    def drain(e, carry):
        @pl.when((chip == 0) | (chip == 2))
        def _():
            copy_to(0, e, tbuf.at[e], 1).wait_send()

        @pl.when(chip == 1)
        def _():
            copy_to(0, e, vbuf.at[e], 1).wait_send()
            copy_to(0, e, vbuf.at[e], 2).wait_send()
        return carry

    def finish_local(c, carry):
        local_copy(c).wait()
        return carry

    def finish_base(c, carry):
        rows = round_rows(c)
        remote(base_out.at[rows], base_out.at[rows], out_send.at[1, c], out_recv.at[1, c], sibling).wait()
        return carry

    relay_early()
    relay_last(0)
    relay_last(1)
    lax.fori_loop(0, NB - 1 - LATE, drain, 0)
    lax.fori_loop(0, NCH - 1, finish_local, 0)
    for e in range(NB - NEED, NB - 2):
        take(e, True)
    take_early()
    take_last(0)
    take_last(1)

    for e in range(NB - 1 - LATE, NB - 2):
        drain(e, 0)

    @pl.when((chip == 0) | (chip == 2))
    def _():
        copy_to(0, NB - 2, tbuf.at[NB - 2], 1).wait_send()

    @pl.when(chip == 1)
    def _():
        copy_to(0, NB - 2, vbuf.at[NB - 2], 2).wait_send()

    @pl.when(chip < 2)
    def _():
        early_copy(0).wait_send()

    for i in range(DUO):
        @pl.when((chip == 0) | (chip == 2))
        def _():
            last_copy(0, i, 1).wait_send()

        @pl.when(chip == 1)
        def _():
            for step in (1, 2):
                vlast_copy(i, step).wait_send()

    local_copy(NCH - 1).wait()
    for c in range(NCH - 1):
        finish_base(c, 0)
    base_copy(0).wait()
    base_copy(1).wait()


def finish(loc_ref, base_ref, out_hbm, stage, sem):
    pieces = []
    for piece in range(PIECES):
        rows = pl.ds(piece * (2 * OWN // PIECES), 2 * OWN // PIECES)
        for k in range(STEPS):
            stage[k, rows, :] = base_ref[rows, :] + loc_ref[k, rows, :]
        pieces.append(pltpu.make_async_copy(stage.at[:, rows], out_hbm.at[:, rows], sem.at[piece]))
        pieces[-1].start()
    for copy in pieces:
        copy.wait()


def solution(mesh):
    vmem = pl.BlockSpec(memory_space=pltpu.VMEM)
    smem = pl.BlockSpec(memory_space=pltpu.SMEM)
    hbm = pl.BlockSpec(memory_space=pltpu.HBM)
    dma = pltpu.SemaphoreType.DMA

    def local(x_init, w_in, w_out, gamma_c, beta_c, gamma_u, beta_u, step_h, guide_w):
        samples, tokens, width = x_init.shape
        rows = samples * tokens
        loc, base = pl.pallas_call(
            kernel,
            out_shape=(jax.ShapeDtypeStruct((STEPS, 2 * NCH, DUO, CH, width), jnp.float32), jax.ShapeDtypeStruct((rows, width), jnp.float32)),
            in_specs=[hbm] * 8 + [smem],
            out_specs=(vmem, vmem),
            scratch_shapes=[
                pltpu.SMEM((STEPS,), jnp.float32),
                pltpu.VMEM((NCH, DUO, CH, WIDTH), jnp.float32),
                pltpu.VMEM((HIDDEN, WIDTH), jnp.bfloat16),
                pltpu.VMEM((PAIR, NCH, DUO, CH, WIDTH), jnp.float32),
                pltpu.VMEM((NCH, DUO, CH, WIDTH), jnp.float32),
                pltpu.VMEM((PAIR, 4, 8, HIDDEN), jnp.float32),
                pltpu.VMEM((PAIR, 8, 128), jnp.float32),
                pltpu.VMEM((4, STEPS, HIDDEN), jnp.bfloat16),
                pltpu.VMEM((4, STEPS, HIDDEN), jnp.bfloat16),
                pltpu.VMEM((4, WIDTH, WIDTH), jnp.bfloat16),
                pltpu.VMEM((DUO, ROWS, WIDTH), jnp.bfloat16),
                pltpu.VMEM((DUO, 4, ROWS, WIDTH), jnp.float32),
                pltpu.VMEM((NB, DUO, CH, WIDTH), jnp.float32),
                pltpu.VMEM((NB, DUO, CH, WIDTH), jnp.float32),
                pltpu.VMEM((2, NB, DUO, CH, WIDTH), jnp.float32),
                pltpu.VMEM((2, DUO, CH, WIDTH), jnp.float32),
                pltpu.VMEM((3, DUO, CH, WIDTH), jnp.float32),
                pltpu.VMEM((DUO, CH, WIDTH), jnp.float32),
                dma((11,)), dma((5,)), dma((5,)), dma((2, NB - 1)), dma((2, NB - 1)), dma((2, NCH)), dma((2, NCH)),
                dma((3, DUO)), dma((3, DUO)), dma((DUO,)), dma((DUO,)), dma((1,)), dma((2,)),
            ],
            compiler_params=pltpu.CompilerParams(collective_id=0, has_side_effects=True, vmem_limit_bytes=48 * 2 ** 20),
            name="picard",
        )(*(pltpu.with_memory_space_constraint(value, pltpu.HBM) for value in (x_init.reshape(2, NCH, DUO, CH, width), w_in, w_out, gamma_c, beta_c, gamma_u, beta_u, step_h)), guide_w)
        out = pl.pallas_call(
            finish,
            out_shape=jax.ShapeDtypeStruct((STEPS, rows, width), jnp.float32),
            in_specs=[vmem] * 2,
            out_specs=hbm,
            scratch_shapes=[pltpu.VMEM((STEPS, rows, width), jnp.float32), dma((PIECES,))],
            compiler_params=pltpu.CompilerParams(vmem_limit_bytes=8 * 2 ** 20),
            name="finish",
        )(loc.reshape(STEPS, rows, width), base)
        return out.reshape(STEPS, samples, tokens, width)

    return jax.shard_map(local, mesh=mesh, in_specs=(P("data", None, None), P(None, None), P(None, None), P("time", None), P("time", None), P("time", None), P("time", None), P("time"), P(None)), out_specs=P("time", "data", None, None), check_vma=False)
```
